128 devices in a mesh: dp: 8 (over x, core), expert: 16 (over y, z).
Axes of the slice: x: 4, y: 4, z: 4, core: 2. Of those that a mesh axis runs over, the one named last changes fastest.
Arguments:
- grads: bfloat16 [131072, 4096], P(('dp', 'expert')), may hold values from -6 to 6
- block_expert: int32 [1024, 1], P(('dp', 'expert')), may hold values from 0 to 15; in each aligned block of 8 rows (0 to 7, 8 to 15, ...) at most 2 rows name the same one
- sketch: bfloat16 [16, 256, 4096], P('expert', None, 'dp'), may hold values from -0.09375 to 0.09375
Outputs:
- factor: bfloat16 [16, 256, 4096], P('expert')
The draws below stay inside these ranges and needn't reach their ends.
Inputs may be any that keep to these rules, and one draw needn't show every extreme that they name: `block_expert`: among the 8 blocks of one device, at most 2 belong to one expert, and every expert has some block.
All inputs are finite; a program needn't handle non-finite values.
Results may differ from the reference program's by a relative error of at most 0.0031.
Values may be sent and summed in bfloat16 or wider, within the bound.
A program may use at most 256 MiB of HBM per device.

```python
import math
import jax
import jax.numpy as jnp
import numpy as np
from jax import lax

D = 4096
L = 256
BLOCK = 128
CAP = 2
ITERS = 5
NBLK = 8
EXPERTS = 16
NBLOCKS = 1024
ROWS = 131072
N_DP = 8


def level_of(rng, extent, shards, least, top_value):
    def one(dim, parts):
        draws = jax.random.uniform(jax.random.fold_in(jax.random.fold_in(rng, 6), dim), (parts,), jnp.float32, least / len(shards), top_value / len(shards))
        return jnp.repeat(jnp.exp(draws), extent[dim] // parts).reshape((-1,) + (1,) * (len(extent) - dim - 1))

    loudness = one(*shards[0])
    for cut in shards[1:]:
        loudness = loudness * one(*cut)
    return loudness


def shared_out(own_key, own, number, rows, amount, top, bound, skew):
    order = jax.random.permutation(own_key, amount)
    packed, ordinary = shares(amount, rows * top, bound, skew, True), shares(amount, rows * top, bound, skew, False)
    places = jnp.arange(amount)

    def named(tallies, rotation):
        used = int((tallies > 0).sum())
        fixed = max(1, used // 4)
        shifted = fixed + (places - fixed + rotation * (used - fixed)) % max(1, amount - fixed)
        return jnp.zeros((amount,), jnp.int32).at[order[jnp.where(places < fixed, places, shifted)]].set(jnp.asarray(tallies, jnp.int32))

    tallies = jnp.where(number % 4 == 0, named(packed, number // 4), named(ordinary, number - number // 4 - 1))
    mixed = jax.random.permutation(jax.random.fold_in(own, 3), amount)
    donor, taker = mixed[0:amount // 2 * 2:2], mixed[1:amount // 2 * 2:2]
    slack = jnp.minimum(tallies[donor] - 1, bound - tallies[taker]) // 2
    slack = jnp.where((donor == order[0]) | (taker == order[0]) | (tallies[taker] == 0), 0, jnp.maximum(slack, 0))
    shifted = jax.random.randint(jax.random.fold_in(own, 4), (amount // 2,), 0, 1 << 20) % (slack + 1)
    tallies = tallies.at[donor].add(-shifted).at[taker].add(shifted)
    members = jnp.searchsorted(jnp.cumsum(tallies), jnp.arange(rows * top), side="right").astype(jnp.int32)
    table = members.reshape(top, rows).T
    table = table[jax.random.permutation(jax.random.fold_in(own, 1), rows)]
    rotation = jax.random.randint(jax.random.fold_in(own, 2), (rows, 1), 0, top)
    return jnp.take_along_axis(table, (jnp.arange(top)[None, :] + rotation) % top, axis=1)


def shares(number_of, total, most, lean, full):
    portions = [(1 << 20) // math.isqrt(rank ** lean) + 1 for rank in range(1, number_of + 1)]
    largest = most if full else min(most, max(-(-total // number_of), total * portions[0] // sum(portions)))
    least = 1 if total - largest >= number_of - 1 else 0
    counts, surplus = [largest] + [least] * (number_of - 1), total - largest - least * (number_of - 1)
    while surplus > 0:
        candidates = [i for i in range(1, number_of) if counts[i] < largest] or [i for i in range(1, number_of) if counts[i] < most]
        whole, budget = sum([portions[i] for i in candidates]), surplus
        for i in candidates:
            extra = min(most - counts[i], max(1, budget * portions[i] // whole), surplus)
            counts[i] = counts[i] + extra
            surplus = surplus - extra
    return np.array(counts)


def scatter_about(rng, dims, deviation, limit, split=(), kind=jnp.bfloat16):
    entries = deviation * jax.random.normal(rng, dims, jnp.float32)
    if split:
        entries = entries * level_of(rng, dims, split, -0.22, 0.18)
    return jnp.clip(entries, -limit, limit).astype(kind)


def setup_inputs(seed: int = 0) -> dict:
    key_list = jax.random.split(jax.random.key(seed), 4)
    grads = scatter_about(key_list[0], (ROWS, D), 1.0, 6.0, ((0, 128),))
    block_expert_keys = jax.random.split(jax.random.fold_in(key_list[1], 1), NBLOCKS // NBLK)
    block_expert_turns = jax.random.permutation(jax.random.fold_in(key_list[1], 3), NBLOCKS // NBLK)
    block_expert = jax.vmap(lambda own, number: shared_out(jax.random.fold_in(key_list[1], 2), own, number, NBLK, EXPERTS, 1, CAP, 2))(block_expert_keys, block_expert_turns).reshape((NBLOCKS, 1))
    sketch = scatter_about(key_list[2], (EXPERTS, L, D), D ** -0.5, 0.09375, ((0, 16), (2, 8)))
    return dict(grads=grads, block_expert=block_expert, sketch=sketch)


EPSILON = 1e-06

def refresh(pair):
    basis, gradient_term = pair
    basis_gram = jnp.dot(basis, basis.T, preferred_element_type=jnp.float32)
    unscaled = jnp.dot(basis_gram, basis.astype(jnp.float32), precision=lax.Precision.HIGHEST)
    unscaled = unscaled + gradient_term / (BLOCK * NBLK * N_DP)
    iterate = unscaled / jnp.sqrt(jnp.sum(unscaled * unscaled) + EPSILON)
    for step in range(ITERS):
        inner = jnp.dot(iterate, iterate.T, precision=lax.Precision.HIGHEST)
        iterate = 1.5 * iterate - 0.5 * jnp.dot(inner, iterate, precision=lax.Precision.HIGHEST)
    return (iterate * math.sqrt(D)).astype(jnp.bfloat16)

def reference(grads, block_expert, sketch):
    count_blocks = block_expert.shape[0]
    blocks = grads.reshape(count_blocks, BLOCK, D)
    owners = block_expert[:, 0].astype(jnp.int32)

    def accumulate(gradient_term, item):
        block_rows, owner = item
        basis = lax.dynamic_index_in_dim(sketch, owner, 0, keepdims=False)
        projected = jnp.dot(basis, block_rows.T, preferred_element_type=jnp.float32).astype(jnp.bfloat16)
        update = jnp.dot(projected, block_rows, preferred_element_type=jnp.float32)
        current = lax.dynamic_index_in_dim(gradient_term, owner, 0, keepdims=False)
        gradient_term = lax.dynamic_update_index_in_dim(gradient_term, current + update, owner, 0)
        return (gradient_term, None)
    start_term = jnp.zeros((EXPERTS, L, D), jnp.float32)
    gradient_term, unused = lax.scan(accumulate, start_term, (blocks, owners))
    return lax.map(refresh, (sketch, gradient_term))
```

```python
import functools

import jax
import jax.numpy as jnp
from jax import lax
from jax.experimental import pallas as pl
from jax.experimental.pallas import tpu as pltpu
from jax.sharding import PartitionSpec as P

D = 4096
L = 256
BLOCK = 128
NBLK = 8
EXPERTS = 16
ITERS = 5
N_DP = 8
COLS = D // N_DP
QUARTER = D // 4
HALF = L // 2
EPSILON = 1e-06
HIGHEST = lax.Precision.HIGHEST
MESH = pl.DeviceIdType.MESH
RING = 4
PARTS = ((0, 48), (48, 48), (96, 32))
ORDERS = ((0, 1, 2), (1, 2, 0), (2, 0, 1))


def mm_nt(a, b):
    return lax.dot_general(a, b, (((1,), (1,)), ((), ())), preferred_element_type=jnp.float32)


def position():
    dp, expert = lax.axis_index("dp"), lax.axis_index("expert")
    return (dp // 2, expert // 4, lax.rem(expert, 4)), lax.rem(dp, 2)


def device(coords, core):
    return (2 * coords[0] + core, 4 * coords[1] + coords[2])


def moved(coords, axis, by):
    return tuple(lax.rem(c + by, RING) if k == axis else c for k, c in enumerate(coords))


def meet(coords, core):
    barrier = pltpu.get_barrier_semaphore()
    peers = [device(moved(coords, a, by), core) for a in range(3) for by in (1, 3)]
    peers.append(device(coords, 1 - core))
    for peer in peers:
        pl.semaphore_signal(barrier, inc=1, device_id=peer, device_id_type=MESH)
    pl.semaphore_wait(barrier, len(peers))


def gather_kernel(sketch_ref, grads_ref, basis_ref, other_ref, send, recv, pair_send, pair_recv, local):
    coords, core = position()
    meet(coords, core)
    partner = device(coords, 1 - core)
    mine = tuple(pl.ds(c, 1) for c in coords)
    cols = pl.ds(pl.multiple_of(core * COLS, COLS), COLS)
    own_rows = pl.ds(pl.multiple_of(core * HALF, HALF), HALF)
    other_rows = pl.ds(pl.multiple_of((1 - core) * HALF, HALF), HALF)
    spot = basis_ref.at[coords[0], coords[1], coords[2], :, cols]
    keep = pltpu.make_async_copy(sketch_ref.at[own_rows], spot, local)
    keep.start()
    give = pltpu.make_async_remote_copy(
        sketch_ref.at[other_rows], spot, pair_send.at[0], pair_recv.at[0], partner, MESH
    )
    give.start()
    swap = pltpu.make_async_remote_copy(
        grads_ref, other_ref, pair_send.at[1], pair_recv.at[1], partner, MESH
    )
    swap.start()
    keep.wait()
    give.wait()

    def view(part, phase, shift, half):
        first, count = PARTS[part]
        order = ORDERS[part]
        index = list(mine)
        for axis in order[:phase]:
            index[axis] = slice(None)
        axis = order[phase]
        index[axis] = pl.ds(lax.rem(coords[axis] + shift, RING), 1)
        columns = slice(None) if half is None else pl.ds(half * (QUARTER // 2), QUARTER // 2)
        return basis_ref.at[index[0], index[1], index[2], pl.ds(first, count), columns]

    def copy(part, phase, which, shift, half, by):
        ref = view(part, phase, shift, half)
        return pltpu.make_async_remote_copy(
            ref,
            ref,
            send.at[part, phase, which],
            recv.at[part, phase, which],
            device(moved(coords, ORDERS[part][phase], by), core),
            MESH,
        )

    def arrived(part, phase, which, shift, half):
        ref = view(part, phase, shift, half)
        pltpu.make_async_copy(ref, ref, recv.at[part, phase, which]).wait()

    sent = []

    def start(*args):
        c = copy(*args)
        c.start()
        sent.append(c)

    for part in range(3):
        start(part, 0, 0, 0, None, 1)
        start(part, 0, 1, 0, None, 3)
    for phase in range(3):
        for part in range(3):
            arrived(part, phase, 0, 3, None)
            start(part, phase, 2, 3, 0, 1)
            arrived(part, phase, 1, 1, None)
            start(part, phase, 3, 1, 1, 3)
        for part in range(3):
            arrived(part, phase, 2, 2, 0)
            arrived(part, phase, 3, 2, 1)
            if phase < 2:
                start(part, phase + 1, 0, 0, None, 1)
                start(part, phase + 1, 1, 0, None, 3)
    for c in sent:
        c.wait_send()
    swap.wait()


def gather(sketch, grads):
    return pl.pallas_call(
        gather_kernel,
        out_shape=(
            jax.ShapeDtypeStruct((4, 4, 4, HALF, QUARTER), jnp.bfloat16),
            jax.ShapeDtypeStruct(grads.shape, jnp.bfloat16),
        ),
        in_specs=[
            pl.BlockSpec(memory_space=pltpu.VMEM),
            pl.BlockSpec(memory_space=pl.ANY),
        ],
        out_specs=(pl.BlockSpec(memory_space=pl.ANY), pl.BlockSpec(memory_space=pl.ANY)),
        scratch_shapes=[
            pltpu.SemaphoreType.DMA((3, 3, 4)),
            pltpu.SemaphoreType.DMA((3, 3, 4)),
            pltpu.SemaphoreType.DMA((2,)),
            pltpu.SemaphoreType.DMA((2,)),
            pltpu.SemaphoreType.DMA,
        ],
        compiler_params=pltpu.CompilerParams(collective_id=0, has_side_effects=True),
    )(sketch, grads)


def term_kernel(count_ref, slot_ref, own_ref, other_ref, s_ref, t_ref, g_ref, p_ref, sem):
    e = pl.program_id(0)
    count = count_ref[e]
    rows_of = NBLK * BLOCK

    @pl.when(e == 0)
    def _():
        first = pltpu.make_async_copy(own_ref, g_ref.at[0:rows_of], sem.at[0])
        second = pltpu.make_async_copy(other_ref, g_ref.at[rows_of : 2 * rows_of], sem.at[1])
        first.start()
        second.start()
        first.wait()
        second.wait()

    def rows(j):
        return pl.ds(pl.multiple_of(slot_ref[4 * e + j] * BLOCK, BLOCK), BLOCK)

    def pair(k, lo, hi):
        return jnp.concatenate([g_ref[rows(2 * k), lo:hi], g_ref[rows(2 * k + 1), lo:hi]], axis=0)

    @pl.when(count == 0)
    def _():
        t_ref[...] = jnp.zeros_like(t_ref)

    for k in range(2):

        @pl.when(count > 2 * k)
        def _(k=k):
            acc = jnp.zeros((HALF, 2 * BLOCK), jnp.float32)
            for x in range(4):
                acc += mm_nt(s_ref[x, 0, 0], pair(k, x * QUARTER, (x + 1) * QUARTER))
            place = lax.broadcasted_iota(jnp.int32, acc.shape, 1) // BLOCK + 2 * k
            p_ref[k] = jnp.where(place < count, acc, 0.0).astype(jnp.bfloat16)

    def emit(pairs):
        for x in range(4):
            for h in range(2):
                lo = x * QUARTER + h * COLS
                total = None
                for k in range(pairs):
                    part = jnp.dot(p_ref[k], pair(k, lo, lo + COLS), preferred_element_type=jnp.float32)
                    total = part if total is None else total + part
                t_ref[x, 0, 0, :, h * COLS : (h + 1) * COLS] = total.astype(jnp.bfloat16)

    pl.when((count > 0) & (count <= 2))(functools.partial(emit, 1))
    pl.when(count > 2)(functools.partial(emit, 2))


def slot_table(owners):
    ids = jnp.arange(EXPERTS, dtype=jnp.int32)
    hit = owners[None, :] == ids[:, None]
    count = jnp.sum(hit.astype(jnp.int32), axis=1)
    blocks = owners.shape[0]
    b = jnp.arange(blocks, dtype=jnp.int32)
    rank = jnp.sum(hit[:, None, :] & (b[None, :] < b[:, None])[None], axis=2).astype(jnp.int32)
    slots = [
        jnp.sum(jnp.where(hit & (rank == j), b[None, :], 0), axis=1) for j in range(4)
    ]
    return count, jnp.stack(slots, axis=1).reshape(-1)


def local_terms(count, slots, basis, grads, other):
    spec = pl.BlockSpec((4, 1, 1, HALF, QUARTER), lambda e, *_: (0, e // 4, e % 4, 0, 0))
    grid_spec = pltpu.PrefetchScalarGridSpec(
        num_scalar_prefetch=2,
        grid=(EXPERTS,),
        in_specs=[pl.BlockSpec(memory_space=pl.ANY), pl.BlockSpec(memory_space=pl.ANY), spec],
        out_specs=spec,
        scratch_shapes=[
            pltpu.VMEM((2 * NBLK * BLOCK, D), jnp.bfloat16),
            pltpu.VMEM((2, HALF, 2 * BLOCK), jnp.bfloat16),
            pltpu.SemaphoreType.DMA((2,)),
        ],
    )
    return pl.pallas_call(
        term_kernel,
        grid_spec=grid_spec,
        out_shape=jax.ShapeDtypeStruct(basis.shape, jnp.bfloat16),
        compiler_params=pltpu.CompilerParams(
            dimension_semantics=("arbitrary",), vmem_limit_bytes=48 * 1024 * 1024
        ),
        cost_estimate=pl.CostEstimate(
            flops=8 * NBLK * BLOCK * HALF * D, bytes_accessed=48 << 20, transcendentals=0
        ),
    )(count, slots, grads, other, basis)


def reduce_kernel(
    t_ref, out_ref, own0, own1, own2, far0, far1, far2, near0, near1, near2,
    mid0, mid1, mid2, fw0, fw1, fw2, mn0, mn1, mn2,
    last0, last1, last2, lf0, lf1, lf2, ln0, ln1, ln2,
    final, send, recv, load, pair_send, pair_recv,
):
    coords, core = position()
    own = (own0, own1, own2)
    far = ((far0, fw0, lf0), (far1, fw1, lf1), (far2, fw2, lf2))
    near = ((near0, mn0, ln0), (near1, mn1, ln1), (near2, mn2, ln2))
    sums = ((None, mid0, last0), (None, mid1, last1), (None, mid2, last2))
    width = QUARTER // 2

    def axis_of(part, phase):
        return ORDERS[part][2 - phase]

    def source(part, phase, shift, half):
        axis = axis_of(part, phase)
        at = lax.rem(coords[axis] + shift, RING)
        columns = pl.ds(half * width, width)
        if phase == 0:
            first, count = PARTS[part]
            index = [slice(None)] * 3
            index[axis] = at
            return t_ref.at[index[0], index[1], index[2], pl.ds(first, count), columns]
        if phase == 1:
            rest = [a for a in range(3) if a != axis_of(part, 0)]
            if rest[0] == axis:
                return sums[part][1].at[at, :, :, columns]
            return sums[part][1].at[:, at, :, columns]
        return sums[part][2].at[at, :, columns]

    loads = []
    for part in range(3):
        for slot, (shift, half) in enumerate(((0, 0), (0, 1), (1, 0), (3, 1))):
            c = pltpu.make_async_copy(
                source(part, 0, shift, half), own[part].at[slot], load.at[part, slot]
            )
            c.start()
            loads.append(c)
    meet(coords, core)
    sent = []

    def push(part, phase, which, src, dst, by):
        c = pltpu.make_async_remote_copy(
            src,
            dst,
            send.at[part, phase, which],
            recv.at[part, phase, which],
            device(moved(coords, axis_of(part, phase), by), core),
            MESH,
        )
        c.start()
        sent.append(c)

    def arrived(part, phase, which, ref):
        pltpu.make_async_copy(ref, ref, recv.at[part, phase, which]).wait()

    def begin(part, phase):
        f, n = far[part][phase], near[part][phase]
        push(part, phase, 0, source(part, phase, 2, 0), f.at[0], 1)
        push(part, phase, 1, source(part, phase, 2, 1), f.at[1], 3)
        push(part, phase, 2, source(part, phase, 1, 1), n.at[1], 1)
        push(part, phase, 3, source(part, phase, 3, 0), n.at[2], 3)

    def held(part, phase, slot):
        if phase == 0:
            return own[part].at[slot]
        shift, half = ((0, 0), (0, 1), (1, 0), (3, 1))[slot]
        return source(part, phase, shift, half)

    def each(phase, fn):
        if phase == 0:

            def body(i, carry):
                fn((lax.div(i, 4), lax.rem(i, 4)))
                return carry

            lax.fori_loop(0, 16, body, 0)
        elif phase == 1:

            def body(i, carry):
                fn((i,))
                return carry

            lax.fori_loop(0, 4, body, 0)
        else:
            fn(())

    def forward(part, phase):
        f, n = far[part][phase], near[part][phase]
        for slot, (which, held_slot, dst, by) in enumerate(((0, 2, 0, 1), (1, 3, 3, 3))):
            arrived(part, phase, which, f.at[slot])
            mine = held(part, phase, held_slot)
            if phase == 0:
                loads[4 * part + held_slot].wait()

            def add(index, slot=slot, mine=mine):
                a = f[(slot, *index)].astype(jnp.float32) + mine[index].astype(jnp.float32)
                f[(slot, *index)] = a.astype(f.dtype)

            each(phase, add)
            push(part, phase, 4 + slot, f.at[slot], n.at[dst], by)

    def finish(part, phase):
        n = near[part][phase]
        arrived(part, phase, 2, n.at[1])
        arrived(part, phase, 3, n.at[2])
        arrived(part, phase, 4, n.at[0])
        arrived(part, phase, 5, n.at[3])
        for half in range(2):
            if phase == 0:
                loads[4 * part + half].wait()
            mine = held(part, phase, half)

            def add(index, half=half, mine=mine):
                a = mine[index].astype(jnp.float32) + n[(half, *index)].astype(jnp.float32)
                a = a + n[(2 + half, *index)].astype(jnp.float32)
                columns = slice(half * width, (half + 1) * width)
                if phase == 2:
                    first, count = PARTS[part]
                    final[half, first : first + count, :] = a
                else:
                    dst = sums[part][phase + 1]
                    dst[(*index, slice(None), columns)] = a.astype(dst.dtype)

            each(phase, add)

    for part in range(3):
        begin(part, 0)
    for phase in range(3):
        for part in range(3):
            forward(part, phase)
        for part in range(3):
            finish(part, phase)
            if phase < 2:
                begin(part, phase + 1)
    swap = pltpu.make_async_remote_copy(
        final.at[1 - core],
        out_ref.at[pl.ds(pl.multiple_of(core * HALF, HALF), HALF)],
        pair_send,
        pair_recv,
        device(coords, 1 - core),
        MESH,
    )
    swap.start()
    out_ref[pl.ds(pl.multiple_of(core * HALF, HALF), HALF), :] = final[core]
    for c in sent:
        c.wait_send()
    swap.wait()


def reduce_terms(partial):
    width = QUARTER // 2
    rows = [count for _, count in PARTS]

    def buffers(lead, dims, dtype):
        return [pltpu.VMEM((*lead, *dims, r, width), dtype) for r in rows]

    def whole(dims, dtype):
        return [pltpu.VMEM((*dims, r, QUARTER), dtype) for r in rows]

    b16, f32 = jnp.bfloat16, jnp.float32
    return pl.pallas_call(
        reduce_kernel,
        out_shape=jax.ShapeDtypeStruct((L, COLS), jnp.float32),
        in_specs=[pl.BlockSpec(memory_space=pl.ANY)],
        out_specs=pl.BlockSpec(memory_space=pltpu.VMEM),
        scratch_shapes=[
            *buffers((4,), (4, 4), b16),
            *buffers((2,), (4, 4), b16),
            *buffers((4,), (4, 4), b16),
            *whole((4, 4), b16),
            *buffers((2,), (4,), b16),
            *buffers((4,), (4,), b16),
            *whole((4,), f32),
            *buffers((2,), (), f32),
            *buffers((4,), (), f32),
            pltpu.VMEM((2, HALF, width), f32),
            pltpu.SemaphoreType.DMA((3, 3, 6)),
            pltpu.SemaphoreType.DMA((3, 3, 6)),
            pltpu.SemaphoreType.DMA((3, 4)),
            pltpu.SemaphoreType.DMA,
            pltpu.SemaphoreType.DMA,
        ],
        compiler_params=pltpu.CompilerParams(
            collective_id=1, has_side_effects=True, vmem_limit_bytes=60 * 1024 * 1024
        ),
    )(partial)


def shards(grads, block_expert, sketch):
    own = sketch[0]
    owners = block_expert[:, 0]
    theirs = lax.ppermute(owners, "dp", [(k, k ^ 1) for k in range(N_DP)])
    basis, other = gather(own, grads)
    count, slots = slot_table(jnp.concatenate([owners, theirs]))
    partial = local_terms(count, slots, basis, grads, other)
    term = reduce_terms(partial)
    basis_gram = lax.psum(mm_nt(own, own), "dp")
    average = float(BLOCK * NBLK * N_DP)
    unscaled = jnp.dot(basis_gram, own.astype(jnp.float32), precision=HIGHEST) + term / average
    gram = lax.psum(
        lax.dot_general(unscaled, unscaled, (((1,), (1,)), ((), ())), precision=HIGHEST), "dp"
    )
    eye = jnp.eye(L, dtype=jnp.float32)
    total = jnp.trace(gram) + EPSILON
    a = gram / total
    q = None
    for step in range(ITERS):
        p = 1.5 * eye - 0.5 * a
        q = p if q is None else jnp.dot(p, q, precision=HIGHEST)
        if step < ITERS - 1:
            a = jnp.dot(jnp.dot(p, a, precision=HIGHEST), p, precision=HIGHEST)
    factor = jnp.dot(q, unscaled * lax.rsqrt(total), precision=HIGHEST) * D**0.5
    return lax.all_gather(factor.astype(jnp.bfloat16), "dp", axis=1, tiled=True)[None]


def solution(mesh):
    in_specs = (P(("dp", "expert"), None), P(("dp", "expert"), None), P("expert", None, "dp"))
    out_specs = P("expert", None, None)
    return jax.shard_map(shards, mesh=mesh, in_specs=in_specs, out_specs=out_specs, check_vma=False)
```

```python
import functools

import jax
import jax.numpy as jnp
from jax import lax
from jax.experimental import pallas as pl
from jax.experimental.pallas import tpu as pltpu
from jax.sharding import PartitionSpec as P

D = 4096
L = 256
BLOCK = 128
NBLK = 8
EXPERTS = 16
ITERS = 5
N_DP = 8
COLS = D // N_DP
QUARTER = D // 4
HALF = L // 2
EPSILON = 1e-06
HIGHEST = lax.Precision.HIGHEST
MESH = pl.DeviceIdType.MESH
RING = 4
PARTS = ((0, 48), (48, 48), (96, 32))
ORDERS = ((0, 1, 2), (1, 2, 0), (2, 0, 1))


def mm_nt(a, b):
    return lax.dot_general(a, b, (((1,), (1,)), ((), ())), preferred_element_type=jnp.float32)


def position():
    dp, expert = lax.axis_index("dp"), lax.axis_index("expert")
    return (dp // 2, expert // 4, lax.rem(expert, 4)), lax.rem(dp, 2)


def device(coords, core):
    return (2 * coords[0] + core, 4 * coords[1] + coords[2])


def moved(coords, axis, by):
    return tuple(lax.rem(c + by, RING) if k == axis else c for k, c in enumerate(coords))


def meet(coords, core, opposite=False):
    barrier = pltpu.get_barrier_semaphore()
    peers = [device(moved(coords, a, by), core) for a in range(3) for by in (1, 3)]
    if opposite:
        peers.append(device(moved(coords, 0, 2), core))
    peers.append(device(coords, 1 - core))
    for peer in peers:
        pl.semaphore_signal(barrier, inc=1, device_id=peer, device_id_type=MESH)
    pl.semaphore_wait(barrier, len(peers))


def gather_kernel(sketch_ref, grads_ref, basis_ref, other_ref, send, recv, pair_send, pair_recv, local):
    coords, core = position()
    meet(coords, core)
    partner = device(coords, 1 - core)
    mine = tuple(pl.ds(c, 1) for c in coords)
    cols = pl.ds(pl.multiple_of(core * COLS, COLS), COLS)
    own_rows = pl.ds(pl.multiple_of(core * HALF, HALF), HALF)
    other_rows = pl.ds(pl.multiple_of((1 - core) * HALF, HALF), HALF)
    spot = basis_ref.at[coords[0], coords[1], coords[2], :, cols]
    keep = pltpu.make_async_copy(sketch_ref.at[own_rows], spot, local)
    keep.start()
    give = pltpu.make_async_remote_copy(
        sketch_ref.at[other_rows], spot, pair_send.at[0], pair_recv.at[0], partner, MESH
    )
    give.start()
    swap = pltpu.make_async_remote_copy(
        grads_ref, other_ref, pair_send.at[1], pair_recv.at[1], partner, MESH
    )
    swap.start()
    keep.wait()
    give.wait()

    def view(part, phase, shift, half):
        first, count = PARTS[part]
        order = ORDERS[part]
        index = list(mine)
        for axis in order[:phase]:
            index[axis] = slice(None)
        axis = order[phase]
        index[axis] = pl.ds(lax.rem(coords[axis] + shift, RING), 1)
        columns = slice(None) if half is None else pl.ds(half * (QUARTER // 2), QUARTER // 2)
        return basis_ref.at[index[0], index[1], index[2], pl.ds(first, count), columns]

    def copy(part, phase, which, shift, half, by):
        ref = view(part, phase, shift, half)
        return pltpu.make_async_remote_copy(
            ref,
            ref,
            send.at[part, phase, which],
            recv.at[part, phase, which],
            device(moved(coords, ORDERS[part][phase], by), core),
            MESH,
        )

    def arrived(part, phase, which, shift, half):
        ref = view(part, phase, shift, half)
        pltpu.make_async_copy(ref, ref, recv.at[part, phase, which]).wait()

    sent = []

    def start(*args):
        c = copy(*args)
        c.start()
        sent.append(c)

    for part in range(3):
        start(part, 0, 0, 0, None, 1)
        start(part, 0, 1, 0, None, 3)
    for phase in range(3):
        for part in range(3):
            arrived(part, phase, 0, 3, None)
            start(part, phase, 2, 3, 0, 1)
            arrived(part, phase, 1, 1, None)
            start(part, phase, 3, 1, 1, 3)
        for part in range(3):
            arrived(part, phase, 2, 2, 0)
            arrived(part, phase, 3, 2, 1)
            if phase < 2:
                start(part, phase + 1, 0, 0, None, 1)
                start(part, phase + 1, 1, 0, None, 3)
    for c in sent:
        c.wait_send()
    swap.wait()


def gather(sketch, grads):
    return pl.pallas_call(
        gather_kernel,
        out_shape=(
            jax.ShapeDtypeStruct((4, 4, 4, HALF, QUARTER), jnp.bfloat16),
            jax.ShapeDtypeStruct(grads.shape, jnp.bfloat16),
        ),
        in_specs=[
            pl.BlockSpec(memory_space=pltpu.VMEM),
            pl.BlockSpec(memory_space=pl.ANY),
        ],
        out_specs=(pl.BlockSpec(memory_space=pl.ANY), pl.BlockSpec(memory_space=pl.ANY)),
        scratch_shapes=[
            pltpu.SemaphoreType.DMA((3, 3, 4)),
            pltpu.SemaphoreType.DMA((3, 3, 4)),
            pltpu.SemaphoreType.DMA((2,)),
            pltpu.SemaphoreType.DMA((2,)),
            pltpu.SemaphoreType.DMA,
        ],
        compiler_params=pltpu.CompilerParams(collective_id=0, has_side_effects=True),
    )(sketch, grads)


def term_kernel(count_ref, slot_ref, own_ref, other_ref, s_ref, t_ref, g_ref, p_ref, sem):
    e = pl.program_id(0)
    count = count_ref[e]
    rows_of = NBLK * BLOCK

    @pl.when(e == 0)
    def _():
        first = pltpu.make_async_copy(own_ref, g_ref.at[0:rows_of], sem.at[0])
        second = pltpu.make_async_copy(other_ref, g_ref.at[rows_of : 2 * rows_of], sem.at[1])
        first.start()
        second.start()
        first.wait()
        second.wait()

    def rows(j):
        return pl.ds(pl.multiple_of(slot_ref[4 * e + j] * BLOCK, BLOCK), BLOCK)

    def pair(k, lo, hi):
        return jnp.concatenate([g_ref[rows(2 * k), lo:hi], g_ref[rows(2 * k + 1), lo:hi]], axis=0)

    @pl.when(count == 0)
    def _():
        t_ref[...] = jnp.zeros_like(t_ref)

    for k in range(2):

        @pl.when(count > 2 * k)
        def _(k=k):
            acc = jnp.zeros((HALF, 2 * BLOCK), jnp.float32)
            for x in range(4):
                acc += mm_nt(s_ref[x, 0, 0], pair(k, x * QUARTER, (x + 1) * QUARTER))
            place = lax.broadcasted_iota(jnp.int32, acc.shape, 1) // BLOCK + 2 * k
            p_ref[k] = jnp.where(place < count, acc, 0.0).astype(jnp.bfloat16)

    def emit(pairs):
        for x in range(4):
            for h in range(2):
                lo = x * QUARTER + h * COLS
                total = None
                for k in range(pairs):
                    part = jnp.dot(p_ref[k], pair(k, lo, lo + COLS), preferred_element_type=jnp.float32)
                    total = part if total is None else total + part
                t_ref[x, 0, 0, :, h * COLS : (h + 1) * COLS] = total.astype(jnp.bfloat16)

    pl.when((count > 0) & (count <= 2))(functools.partial(emit, 1))
    pl.when(count > 2)(functools.partial(emit, 2))


def slot_table(owners):
    ids = jnp.arange(EXPERTS, dtype=jnp.int32)
    hit = owners[None, :] == ids[:, None]
    count = jnp.sum(hit.astype(jnp.int32), axis=1)
    blocks = owners.shape[0]
    b = jnp.arange(blocks, dtype=jnp.int32)
    rank = jnp.sum(hit[:, None, :] & (b[None, :] < b[:, None])[None], axis=2).astype(jnp.int32)
    slots = [
        jnp.sum(jnp.where(hit & (rank == j), b[None, :], 0), axis=1) for j in range(4)
    ]
    return count, jnp.stack(slots, axis=1).reshape(-1)


def local_terms(count, slots, basis, grads, other):
    spec = pl.BlockSpec((4, 1, 1, HALF, QUARTER), lambda e, *_: (0, e // 4, e % 4, 0, 0))
    grid_spec = pltpu.PrefetchScalarGridSpec(
        num_scalar_prefetch=2,
        grid=(EXPERTS,),
        in_specs=[pl.BlockSpec(memory_space=pl.ANY), pl.BlockSpec(memory_space=pl.ANY), spec],
        out_specs=spec,
        scratch_shapes=[
            pltpu.VMEM((2 * NBLK * BLOCK, D), jnp.bfloat16),
            pltpu.VMEM((2, HALF, 2 * BLOCK), jnp.bfloat16),
            pltpu.SemaphoreType.DMA((2,)),
        ],
    )
    return pl.pallas_call(
        term_kernel,
        grid_spec=grid_spec,
        out_shape=jax.ShapeDtypeStruct(basis.shape, jnp.bfloat16),
        compiler_params=pltpu.CompilerParams(
            dimension_semantics=("arbitrary",), vmem_limit_bytes=48 * 1024 * 1024
        ),
        cost_estimate=pl.CostEstimate(
            flops=8 * NBLK * BLOCK * HALF * D, bytes_accessed=48 << 20, transcendentals=0
        ),
    )(count, slots, grads, other, basis)


def reduce_kernel(
    t_ref, gram_ref, sketch_ref, out_ref, own0, own1, own2, far0, far1, far2, near0, near1, near2,
    mid0, mid1, mid2, fw0, fw1, fw2, mn0, mn1, mn2,
    last0, last1, last2, lf0, lf1, lf2, ln0, ln1, ln2,
    final, term, gp, gin, gx, gfull, send, recv, load, pair_send, pair_recv, x_send, x_recv,
):
    coords, core = position()
    own = (own0, own1, own2)
    far = ((far0, fw0, lf0), (far1, fw1, lf1), (far2, fw2, lf2))
    near = ((near0, mn0, ln0), (near1, mn1, ln1), (near2, mn2, ln2))
    sums = ((None, mid0, last0), (None, mid1, last1), (None, mid2, last2))
    width = QUARTER // 2

    def axis_of(part, phase):
        return ORDERS[part][2 - phase]

    def source(part, phase, shift, half):
        axis = axis_of(part, phase)
        at = lax.rem(coords[axis] + shift, RING)
        columns = pl.ds(half * width, width)
        if phase == 0:
            first, count = PARTS[part]
            index = [slice(None)] * 3
            index[axis] = at
            return t_ref.at[index[0], index[1], index[2], pl.ds(first, count), columns]
        if phase == 1:
            rest = [a for a in range(3) if a != axis_of(part, 0)]
            if rest[0] == axis:
                return sums[part][1].at[at, :, :, columns]
            return sums[part][1].at[:, at, :, columns]
        return sums[part][2].at[at, :, columns]

    loads = []
    for part in range(3):
        for slot, (shift, half) in enumerate(((0, 0), (0, 1), (1, 0), (3, 1))):
            c = pltpu.make_async_copy(
                source(part, 0, shift, half), own[part].at[slot], load.at[part, slot]
            )
            c.start()
            loads.append(c)
    meet(coords, core, opposite=True)
    sent = []

    def push(part, phase, which, src, dst, by):
        c = pltpu.make_async_remote_copy(
            src,
            dst,
            send.at[part, phase, which],
            recv.at[part, phase, which],
            device(moved(coords, axis_of(part, phase), by), core),
            MESH,
        )
        c.start()
        sent.append(c)

    def arrived(part, phase, which, ref):
        pltpu.make_async_copy(ref, ref, recv.at[part, phase, which]).wait()

    def begin(part, phase):
        f, n = far[part][phase], near[part][phase]
        push(part, phase, 0, source(part, phase, 2, 0), f.at[0], 1)
        push(part, phase, 1, source(part, phase, 2, 1), f.at[1], 3)
        push(part, phase, 2, source(part, phase, 1, 1), n.at[1], 1)
        push(part, phase, 3, source(part, phase, 3, 0), n.at[2], 3)

    def held(part, phase, slot):
        if phase == 0:
            return own[part].at[slot]
        shift, half = ((0, 0), (0, 1), (1, 0), (3, 1))[slot]
        return source(part, phase, shift, half)

    def each(phase, fn):
        if phase == 0:

            def body(i, carry):
                fn((lax.div(i, 4), lax.rem(i, 4)))
                return carry

            lax.fori_loop(0, 16, body, 0)
        elif phase == 1:

            def body(i, carry):
                fn((i,))
                return carry

            lax.fori_loop(0, 4, body, 0)
        else:
            fn(())

    def forward(part, phase):
        f, n = far[part][phase], near[part][phase]
        for slot, (which, held_slot, dst, by) in enumerate(((0, 2, 0, 1), (1, 3, 3, 3))):
            arrived(part, phase, which, f.at[slot])
            mine = held(part, phase, held_slot)
            if phase == 0:
                loads[4 * part + held_slot].wait()

            def add(index, slot=slot, mine=mine):
                a = f[(slot, *index)].astype(jnp.float32) + mine[index].astype(jnp.float32)
                f[(slot, *index)] = a.astype(f.dtype)

            each(phase, add)
            push(part, phase, 4 + slot, f.at[slot], n.at[dst], by)

    def finish(part, phase):
        n = near[part][phase]
        arrived(part, phase, 2, n.at[1])
        arrived(part, phase, 3, n.at[2])
        arrived(part, phase, 4, n.at[0])
        arrived(part, phase, 5, n.at[3])
        for half in range(2):
            if phase == 0:
                loads[4 * part + half].wait()
            mine = held(part, phase, half)

            def add(index, half=half, mine=mine):
                a = mine[index].astype(jnp.float32) + n[(half, *index)].astype(jnp.float32)
                a = a + n[(2 + half, *index)].astype(jnp.float32)
                columns = slice(half * width, (half + 1) * width)
                if phase == 2:
                    first, count = PARTS[part]
                    final[half, first : first + count, :] = a
                else:
                    dst = sums[part][phase + 1]
                    dst[(*index, slice(None), columns)] = a.astype(dst.dtype)

            each(phase, add)

    for part in range(3):
        begin(part, 0)
    for phase in range(3):
        for part in range(3):
            forward(part, phase)
        for part in range(3):
            finish(part, phase)
            if phase < 2:
                begin(part, phase + 1)
    partner = device(coords, 1 - core)
    mine = pl.ds(pl.multiple_of(core * HALF, HALF), HALF)
    theirs = pl.ds(pl.multiple_of((1 - core) * HALF, HALF), HALF)

    def give(src, dst, which):
        c = pltpu.make_async_remote_copy(
            src, dst, pair_send.at[which], pair_recv.at[which], partner, MESH
        )
        c.start()
        return c

    def across(src, dst, which, by):
        c = pltpu.make_async_remote_copy(
            src, dst, x_send.at[which], x_recv.at[which], device(moved(coords, 0, by), core), MESH
        )
        c.start()
        return c

    swap = give(final.at[1 - core], term.at[mine], 0)
    term[mine, :] = final[core]
    product = two_pass(gram_ref[...], sketch_ref[...])
    swap.wait()
    average = float(BLOCK * NBLK * N_DP)
    unscaled = product + term[...] / average
    term[...] = unscaled
    gp[...] = three_pass_nt(unscaled, unscaled)
    swap = give(gp.at[theirs], gin, 1)
    swap.wait()
    gin[...] = gin[...] + gp[mine, :]
    sends = [across(gin, gx.at[by - 1], by - 1, by) for by in (1, 2, 3)]
    for c in sends:
        c.wait()
    gfull[mine, :] = (gin[...] + gx[1]) + (gx[0] + gx[2])
    swap = give(gfull.at[mine], gfull.at[mine], 2)
    swap.wait()
    gram = gfull[...]
    row = lax.broadcasted_iota(jnp.int32, (L, L), 0)
    col = lax.broadcasted_iota(jnp.int32, (L, L), 1)
    diagonal = row == col
    total = jnp.sum(jnp.where(diagonal, gram, 0.0)) + EPSILON
    total = jnp.full((1, 1), total, jnp.float32)
    a = gram / total
    q = None
    for step in range(ITERS):
        p = jnp.where(diagonal, 1.5, 0.0) - 0.5 * a
        q = p if q is None else three_pass(p, q)
        if step < ITERS - 1:
            a = three_pass(three_pass(p, a), p)
    scale = D**0.5 * lax.rsqrt(total)
    factor = three_pass(q, term[...] * scale)

    def chunk(shift, core_of):
        index = 2 * lax.rem(coords[0] + shift, RING) + core_of
        return pl.ds(pl.multiple_of(index * COLS, COLS), COLS)

    def piece(shift, rows=slice(None)):
        return out_ref.at[rows, chunk(shift, core)]

    out_ref[:, chunk(0, core)] = factor.astype(jnp.bfloat16)
    upper, lower = pl.ds(0, HALF), pl.ds(HALF, HALF)
    right = across(piece(0), piece(0), 3, 1)
    left = across(piece(0), piece(0), 4, 3)
    gives = [give(piece(0), piece(0), 3)]
    right.wait_recv()
    on_right = across(piece(3, upper), piece(3, upper), 5, 1)
    gives.append(give(piece(3), piece(3), 4))
    left.wait_recv()
    on_left = across(piece(1, lower), piece(1, lower), 6, 3)
    gives.append(give(piece(1), piece(1), 5))
    on_right.wait_recv()
    gives.append(give(piece(2, upper), piece(2, upper), 6))
    on_left.wait_recv()
    gives.append(give(piece(2, lower), piece(2, lower), 7))
    for c in (right, left, on_right, on_left):
        c.wait_send()
    for c in gives:
        c.wait()
    for c in sent:
        c.wait_send()


def split(a):
    high = a.astype(jnp.bfloat16)
    return high, (a - high.astype(jnp.float32)).astype(jnp.bfloat16)


def mm(a, b):
    return jnp.dot(a, b, preferred_element_type=jnp.float32)


def two_pass(a, b):
    high, low = split(a)
    return mm(high, b) + mm(low, b)


def three_pass(a, b):
    ah, al = split(a)
    bh, bl = split(b)
    return mm(ah, bh) + (mm(ah, bl) + mm(al, bh))


def three_pass_nt(a, b):
    ah, al = split(a)
    bh, bl = split(b)
    return mm_nt(ah, bh) + (mm_nt(ah, bl) + mm_nt(al, bh))


def reduce_terms(partial, basis_gram, own):
    width = QUARTER // 2
    rows = [count for _, count in PARTS]

    def buffers(lead, dims, dtype):
        return [pltpu.VMEM((*lead, *dims, r, width), dtype) for r in rows]

    def whole(dims, dtype):
        return [pltpu.VMEM((*dims, r, QUARTER), dtype) for r in rows]

    b16, f32 = jnp.bfloat16, jnp.float32
    return pl.pallas_call(
        reduce_kernel,
        out_shape=jax.ShapeDtypeStruct((L, D), jnp.bfloat16),
        in_specs=[
            pl.BlockSpec(memory_space=pl.ANY),
            pl.BlockSpec(memory_space=pltpu.VMEM),
            pl.BlockSpec(memory_space=pltpu.VMEM),
        ],
        out_specs=pl.BlockSpec(memory_space=pltpu.VMEM),
        scratch_shapes=[
            *buffers((4,), (4, 4), b16),
            *buffers((2,), (4, 4), b16),
            *buffers((4,), (4, 4), b16),
            *whole((4, 4), b16),
            *buffers((2,), (4,), b16),
            *buffers((4,), (4,), b16),
            *whole((4,), f32),
            *buffers((2,), (), f32),
            *buffers((4,), (), f32),
            pltpu.VMEM((2, HALF, width), f32),
            pltpu.VMEM((L, COLS), f32),
            pltpu.VMEM((L, L), f32),
            pltpu.VMEM((HALF, L), f32),
            pltpu.VMEM((3, HALF, L), f32),
            pltpu.VMEM((L, L), f32),
            pltpu.SemaphoreType.DMA((3, 3, 6)),
            pltpu.SemaphoreType.DMA((3, 3, 6)),
            pltpu.SemaphoreType.DMA((3, 4)),
            pltpu.SemaphoreType.DMA((8,)),
            pltpu.SemaphoreType.DMA((8,)),
            pltpu.SemaphoreType.DMA((7,)),
            pltpu.SemaphoreType.DMA((7,)),
        ],
        compiler_params=pltpu.CompilerParams(
            collective_id=1, has_side_effects=True, vmem_limit_bytes=60 * 1024 * 1024
        ),
    )(partial, basis_gram, own)


def shards(grads, block_expert, sketch):
    own = sketch[0]
    owners = block_expert[:, 0]
    theirs = lax.ppermute(owners, "dp", [(k, k ^ 1) for k in range(N_DP)])
    basis_gram = lax.psum(mm_nt(own, own), "dp")
    basis, other = gather(own, grads)
    count, slots = slot_table(jnp.concatenate([owners, theirs]))
    partial = local_terms(count, slots, basis, grads, other)
    return reduce_terms(partial, basis_gram, own)[None]


def solution(mesh):
    in_specs = (P(("dp", "expert"), None), P(("dp", "expert"), None), P("expert", None, "dp"))
    out_specs = P("expert", None, None)
    return jax.shard_map(shards, mesh=mesh, in_specs=in_specs, out_specs=out_specs, check_vma=False)
```

```python
import functools

import jax
import jax.numpy as jnp
from jax import lax
from jax.experimental import pallas as pl
from jax.experimental.pallas import tpu as pltpu
from jax.sharding import PartitionSpec as P

D = 4096
L = 256
BLOCK = 128
NBLK = 8
EXPERTS = 16
ITERS = 5
N_DP = 8
COLS = D // N_DP
QUARTER = D // 4
HALF = L // 2
EPSILON = 1e-06
HIGHEST = lax.Precision.HIGHEST
MESH = pl.DeviceIdType.MESH
RING = 4
PARTS = ((0, 48), (48, 48), (96, 32))
ORDERS = ((0, 1, 2), (1, 2, 0), (2, 0, 1))


def mm_nt(a, b):
    return lax.dot_general(a, b, (((1,), (1,)), ((), ())), preferred_element_type=jnp.float32)


def position():
    dp, expert = lax.axis_index("dp"), lax.axis_index("expert")
    return (dp // 2, expert // 4, lax.rem(expert, 4)), lax.rem(dp, 2)


def device(coords, core):
    return (2 * coords[0] + core, 4 * coords[1] + coords[2])


def moved(coords, axis, by):
    return tuple(lax.rem(c + by, RING) if k == axis else c for k, c in enumerate(coords))


def meet(coords, core, opposite=False):
    barrier = pltpu.get_barrier_semaphore()
    peers = [device(moved(coords, a, by), core) for a in range(3) for by in (1, 3)]
    if opposite:
        peers.append(device(moved(coords, 0, 2), core))
    peers.append(device(coords, 1 - core))
    for peer in peers:
        pl.semaphore_signal(barrier, inc=1, device_id=peer, device_id_type=MESH)
    pl.semaphore_wait(barrier, len(peers))


PIECES = tuple((32 * k, 32, 0, QUARTER, ORDERS[k], True) for k in range(3)) + tuple(
    (96, 32, first, count, ORDERS[k], False)
    for k, (first, count) in enumerate(((0, 384), (384, 384), (768, 256)))
)
GATHER_COPIES = 4 * sum(6 if piece[5] else 3 for piece in PIECES)
ALL = slice(None)


class GatherRing:
    def __init__(self, env, piece, fixed, axis):
        self.env, self.piece, self.fixed, self.axis = env, piece, fixed, axis
        self.ids = [env["count"] + k for k in range(4)]
        env["count"] += 4

    def view(self, shift, half=None):
        coords = self.env["coords"]
        row, rows, col, cols = self.piece[:4]
        if half is not None:
            row, rows = row + half * (rows // 2), rows // 2
        index = []
        for axis in range(3):
            step = shift if axis == self.axis else self.fixed.get(axis, 0)
            index.append(ALL if step is ALL else pl.ds(lax.rem(coords[axis] + step, RING), 1))
        return self.env["ref"].at[(*index, pl.ds(row, rows), pl.ds(col, cols))]

    def push(self, which, ref, by):
        env, k = self.env, self.ids[which]
        target = device(moved(env["coords"], self.axis, by), env["core"])
        copy = pltpu.make_async_remote_copy(
            ref, ref, env["send"].at[k], env["recv"].at[k], target, MESH
        )
        copy.start()
        env["sent"].append(copy)

    def arrived(self, which, ref):
        pltpu.make_async_copy(ref, ref, self.env["recv"].at[self.ids[which]]).wait()

    def start(self):
        self.push(0, self.view(0), 1)
        self.push(1, self.view(0), 3)

    def forward(self):
        self.arrived(0, self.view(3))
        self.push(2, self.view(3, 0), 1)
        self.arrived(1, self.view(1))
        self.push(3, self.view(1, 1), 3)

    def finish(self):
        self.arrived(2, self.view(2, 0))
        self.arrived(3, self.view(2, 1))


def gather_kernel(sketch_ref, grads_ref, basis_ref, other_ref, send, recv, pair_send, pair_recv, local):
    coords, core = position()
    meet(coords, core)
    partner = device(coords, 1 - core)
    cols = pl.ds(pl.multiple_of(core * COLS, COLS), COLS)
    own_rows = pl.ds(pl.multiple_of(core * HALF, HALF), HALF)
    other_rows = pl.ds(pl.multiple_of((1 - core) * HALF, HALF), HALF)
    spot = basis_ref.at[coords[0], coords[1], coords[2], :, cols]
    keep = pltpu.make_async_copy(sketch_ref.at[own_rows], spot, local)
    keep.start()
    give = pltpu.make_async_remote_copy(
        sketch_ref.at[other_rows], spot, pair_send.at[0], pair_recv.at[0], partner, MESH
    )
    give.start()
    swap = pltpu.make_async_remote_copy(
        grads_ref, other_ref, pair_send.at[1], pair_recv.at[1], partner, MESH
    )
    keep.wait()
    give.wait()

    env = dict(coords=coords, core=core, ref=basis_ref, send=send, recv=recv, sent=[], count=0)
    first, second, third = [], [], []
    for piece in PIECES:
        a1, a2, a3 = piece[4]
        first.append(GatherRing(env, piece, {}, a1))
        second.append(GatherRing(env, piece, {a1: ALL}, a2))
        steps = (0, 3, 1, 2) if piece[5] else (ALL,)
        third.append([GatherRing(env, piece, {a1: ALL, a2: k}, a3) for k in steps])
    sliced = [k for k, piece in enumerate(PIECES) if piece[5]]
    for ring in first:
        ring.start()
    swap.start()
    for ring in first:
        ring.forward()
    for k, ring in enumerate(first):
        ring.finish()
        second[k].start()
    for k in sliced:
        third[k][0].start()
    for ring in second:
        ring.forward()
    for k in sliced:
        third[k][1].start()
        third[k][2].start()
    for k in sliced:
        third[k][0].forward()
    for k, ring in enumerate(second):
        ring.finish()
        third[k][-1].start()
    for step in (1, 2, 3):
        for k in sliced:
            third[k][step].forward()
    for k in range(len(PIECES)):
        if k not in sliced:
            third[k][0].forward()
    for rings in third:
        for ring in rings:
            ring.finish()
    for copy in env["sent"]:
        copy.wait_send()
    swap.wait()


def gather(sketch, grads):
    return pl.pallas_call(
        gather_kernel,
        out_shape=(
            jax.ShapeDtypeStruct((4, 4, 4, HALF, QUARTER), jnp.bfloat16),
            jax.ShapeDtypeStruct(grads.shape, jnp.bfloat16),
        ),
        in_specs=[
            pl.BlockSpec(memory_space=pltpu.VMEM),
            pl.BlockSpec(memory_space=pl.ANY),
        ],
        out_specs=(pl.BlockSpec(memory_space=pl.ANY), pl.BlockSpec(memory_space=pl.ANY)),
        scratch_shapes=[
            pltpu.SemaphoreType.DMA((GATHER_COPIES,)),
            pltpu.SemaphoreType.DMA((GATHER_COPIES,)),
            pltpu.SemaphoreType.DMA((2,)),
            pltpu.SemaphoreType.DMA((2,)),
            pltpu.SemaphoreType.DMA,
        ],
        compiler_params=pltpu.CompilerParams(collective_id=0, has_side_effects=True),
    )(sketch, grads)


def term_kernel(count_ref, slot_ref, order_ref, own_ref, other_ref, s_ref, t_ref, g_ref, p_ref, sem):
    e = pl.program_id(0)
    count = count_ref[e]

    def block_copy(b, src):
        rows = pl.ds(pl.multiple_of(lax.rem(b, NBLK) * BLOCK, BLOCK), BLOCK)
        place = pl.ds(pl.multiple_of(b * BLOCK, BLOCK), BLOCK)
        return pltpu.make_async_copy(src.at[rows], g_ref.at[place], sem.at[b])

    @pl.when(e == 0)
    def _():
        for k in range(2 * NBLK):
            b = order_ref[k]

            @pl.when(b < NBLK)
            def _(b=b):
                block_copy(b, own_ref).start()

            @pl.when(b >= NBLK)
            def _(b=b):
                block_copy(b, other_ref).start()

    for j in range(4):

        @pl.when(count > j)
        def _(j=j):
            block_copy(slot_ref[4 * e + j], own_ref).wait()

    def rows(j):
        return pl.ds(pl.multiple_of(slot_ref[4 * e + j] * BLOCK, BLOCK), BLOCK)

    def pair(k, lo, hi):
        return jnp.concatenate([g_ref[rows(2 * k), lo:hi], g_ref[rows(2 * k + 1), lo:hi]], axis=0)

    @pl.when(count == 0)
    def _():
        t_ref[...] = jnp.zeros_like(t_ref)

    for k in range(2):

        @pl.when(count > 2 * k)
        def _(k=k):
            acc = jnp.zeros((2 * BLOCK, HALF), jnp.float32)
            for x in range(4):
                acc += mm_nt(pair(k, x * QUARTER, (x + 1) * QUARTER), s_ref[x, 0, 0])
            place = lax.broadcasted_iota(jnp.int32, acc.shape, 0) // BLOCK + 2 * k
            p_ref[k] = jnp.where(place < count, acc, 0.0).T.astype(jnp.bfloat16)

    def emit(pairs):
        for x in range(4):
            for h in range(2):
                lo = x * QUARTER + h * COLS
                total = None
                for k in range(pairs):
                    part = jnp.dot(p_ref[k], pair(k, lo, lo + COLS), preferred_element_type=jnp.float32)
                    total = part if total is None else total + part
                t_ref[x, 0, 0, :, h * COLS : (h + 1) * COLS] = total.astype(jnp.bfloat16)

    pl.when((count > 0) & (count <= 2))(functools.partial(emit, 1))
    pl.when(count > 2)(functools.partial(emit, 2))


def slot_table(owners):
    ids = jnp.arange(EXPERTS, dtype=jnp.int32)
    hit = owners[None, :] == ids[:, None]
    count = jnp.sum(hit.astype(jnp.int32), axis=1)
    blocks = owners.shape[0]
    b = jnp.arange(blocks, dtype=jnp.int32)
    rank = jnp.sum(hit[:, None, :] & (b[None, :] < b[:, None])[None], axis=2).astype(jnp.int32)
    slot0 = jnp.sum(jnp.where(hit & (rank == 0), b[None, :], 0), axis=1)
    slots = [
        jnp.where(count > j, jnp.sum(jnp.where(hit & (rank == j), b[None, :], 0), axis=1), slot0)
        for j in range(4)
    ]
    key = owners * blocks + b
    turn = jnp.sum((key[None, :] < key[:, None]).astype(jnp.int32), axis=1)
    order = jnp.sum(jnp.where(turn[None, :] == b[:, None], b[None, :], 0), axis=1)
    return count, jnp.stack(slots, axis=1).reshape(-1), order


def local_terms(count, slots, order, basis, grads, other):
    spec = pl.BlockSpec((4, 1, 1, HALF, QUARTER), lambda e, *_: (0, e // 4, e % 4, 0, 0))
    grid_spec = pltpu.PrefetchScalarGridSpec(
        num_scalar_prefetch=3,
        grid=(EXPERTS,),
        in_specs=[pl.BlockSpec(memory_space=pl.ANY), pl.BlockSpec(memory_space=pl.ANY), spec],
        out_specs=spec,
        scratch_shapes=[
            pltpu.VMEM((2 * NBLK * BLOCK, D), jnp.bfloat16),
            pltpu.VMEM((2, HALF, 2 * BLOCK), jnp.bfloat16),
            pltpu.SemaphoreType.DMA((2 * NBLK,)),
        ],
    )
    return pl.pallas_call(
        term_kernel,
        grid_spec=grid_spec,
        out_shape=jax.ShapeDtypeStruct(basis.shape, jnp.bfloat16),
        compiler_params=pltpu.CompilerParams(
            dimension_semantics=("arbitrary",), vmem_limit_bytes=48 * 1024 * 1024
        ),
        cost_estimate=pl.CostEstimate(
            flops=8 * NBLK * BLOCK * HALF * D, bytes_accessed=48 << 20, transcendentals=0
        ),
    )(count, slots, order, grads, other, basis)


def reduce_kernel(
    t_ref, basis_ref, sketch_ref, out_ref, own0, own1, own2, far0, far1, far2, near0, near1, near2,
    mid0, mid1, mid2, fw0, fw1, fw2, mn0, mn1, mn2,
    last0, last1, last2, lf0, lf1, lf2, ln0, ln1, ln2,
    final, whole, term, gp, gin, gx, gfull, send, recv, load, pair_send, pair_recv, x_send, x_recv,
):
    coords, core = position()
    own = (own0, own1, own2)
    far = ((far0, fw0, lf0), (far1, fw1, lf1), (far2, fw2, lf2))
    near = ((near0, mn0, ln0), (near1, mn1, ln1), (near2, mn2, ln2))
    sums = ((None, mid0, last0), (None, mid1, last1), (None, mid2, last2))
    width = QUARTER // 2

    def axis_of(part, phase):
        return ORDERS[part][2 - phase]

    def source(part, phase, shift, half):
        axis = axis_of(part, phase)
        at = lax.rem(coords[axis] + shift, RING)
        columns = pl.ds(half * width, width)
        if phase == 0:
            first, count = PARTS[part]
            index = [slice(None)] * 3
            index[axis] = at
            return t_ref.at[index[0], index[1], index[2], pl.ds(first, count), columns]
        if phase == 1:
            rest = [a for a in range(3) if a != axis_of(part, 0)]
            if rest[0] == axis:
                return sums[part][1].at[at, :, :, columns]
            return sums[part][1].at[:, at, :, columns]
        return sums[part][2].at[at, :, columns]

    loads = []
    for part in range(3):
        for slot, (shift, half) in enumerate(((0, 0), (0, 1), (1, 0), (3, 1))):
            c = pltpu.make_async_copy(
                source(part, 0, shift, half), own[part].at[slot], load.at[part, slot]
            )
            c.start()
            loads.append(c)
    whole_own = pltpu.make_async_copy(
        basis_ref.at[:, coords[1], coords[2]], whole.at[core], load.at[3, 0]
    )
    whole_own.start()
    meet(coords, core, opposite=True)
    sent = []

    def push(part, phase, which, src, dst, by):
        c = pltpu.make_async_remote_copy(
            src,
            dst,
            send.at[part, phase, which],
            recv.at[part, phase, which],
            device(moved(coords, axis_of(part, phase), by), core),
            MESH,
        )
        c.start()
        sent.append(c)

    def arrived(part, phase, which, ref):
        pltpu.make_async_copy(ref, ref, recv.at[part, phase, which]).wait()

    def begin(part, phase):
        f, n = far[part][phase], near[part][phase]
        push(part, phase, 0, source(part, phase, 2, 0), f.at[0], 1)
        push(part, phase, 1, source(part, phase, 2, 1), f.at[1], 3)
        push(part, phase, 2, source(part, phase, 1, 1), n.at[1], 1)
        push(part, phase, 3, source(part, phase, 3, 0), n.at[2], 3)

    def held(part, phase, slot):
        if phase == 0:
            return own[part].at[slot]
        shift, half = ((0, 0), (0, 1), (1, 0), (3, 1))[slot]
        return source(part, phase, shift, half)

    def each(phase, fn):
        if phase == 0:

            def body(i, carry):
                fn((lax.div(i, 4), lax.rem(i, 4)))
                return carry

            lax.fori_loop(0, 16, body, 0)
        elif phase == 1:

            def body(i, carry):
                fn((i,))
                return carry

            lax.fori_loop(0, 4, body, 0)
        else:
            fn(())

    def forward(part, phase):
        f, n = far[part][phase], near[part][phase]
        for slot, (which, held_slot, dst, by) in enumerate(((0, 2, 0, 1), (1, 3, 3, 3))):
            arrived(part, phase, which, f.at[slot])
            mine = held(part, phase, held_slot)
            if phase == 0:
                loads[4 * part + held_slot].wait()

            def add(index, slot=slot, mine=mine):
                a = f[(slot, *index)].astype(jnp.float32) + mine[index].astype(jnp.float32)
                f[(slot, *index)] = a.astype(f.dtype)

            each(phase, add)
            push(part, phase, 4 + slot, f.at[slot], n.at[dst], by)

    def finish(part, phase):
        n = near[part][phase]
        arrived(part, phase, 2, n.at[1])
        arrived(part, phase, 3, n.at[2])
        arrived(part, phase, 4, n.at[0])
        arrived(part, phase, 5, n.at[3])
        for half in range(2):
            if phase == 0:
                loads[4 * part + half].wait()
            mine = held(part, phase, half)

            def add(index, half=half, mine=mine):
                a = mine[index].astype(jnp.float32) + n[(half, *index)].astype(jnp.float32)
                a = a + n[(2 + half, *index)].astype(jnp.float32)
                columns = slice(half * width, (half + 1) * width)
                if phase == 2:
                    first, count = PARTS[part]
                    final[half, first : first + count, :] = a
                else:
                    dst = sums[part][phase + 1]
                    dst[(*index, slice(None), columns)] = a.astype(dst.dtype)

            each(phase, add)

    for part in range(3):
        begin(part, 0)
    whole_swap = pltpu.make_async_remote_copy(
        basis_ref.at[:, coords[1], coords[2]],
        whole.at[core],
        pair_send.at[8],
        pair_recv.at[8],
        device(coords, 1 - core),
        MESH,
    )
    whole_swap.start()
    whole_own.wait()
    whole_swap.wait()
    gp[...] = jnp.zeros_like(gp)
    for x in range(4):
        for h in range(2):
            gp[h * HALF : (h + 1) * HALF, 0:HALF] += mm_nt(whole[h, x], whole[0, x])
            gp[h * HALF : (h + 1) * HALF, HALF:] += mm_nt(whole[h, x], whole[1, x])
    for phase in range(3):
        for part in range(3):
            forward(part, phase)
        for part in range(3):
            finish(part, phase)
            if phase < 2:
                begin(part, phase + 1)
    partner = device(coords, 1 - core)
    mine = pl.ds(pl.multiple_of(core * HALF, HALF), HALF)
    theirs = pl.ds(pl.multiple_of((1 - core) * HALF, HALF), HALF)

    def give(src, dst, which):
        c = pltpu.make_async_remote_copy(
            src, dst, pair_send.at[which], pair_recv.at[which], partner, MESH
        )
        c.start()
        return c

    def across(src, dst, which, by):
        c = pltpu.make_async_remote_copy(
            src, dst, x_send.at[which], x_recv.at[which], device(moved(coords, 0, by), core), MESH
        )
        c.start()
        return c

    swap = give(final.at[1 - core], term.at[mine], 0)
    term[mine, :] = final[core]
    product = two_pass(gp[...], sketch_ref[...])
    swap.wait()
    average = float(BLOCK * NBLK * N_DP)
    unscaled = product + term[...] / average
    term[...] = unscaled
    gp[...] = three_pass_nt(unscaled, unscaled)
    swap = give(gp.at[theirs], gin, 1)
    swap.wait()
    gin[...] = gin[...] + gp[mine, :]
    sends = [across(gin, gx.at[by - 1], by - 1, by) for by in (1, 2, 3)]
    for c in sends:
        c.wait()
    gfull[mine, :] = (gin[...] + gx[1]) + (gx[0] + gx[2])
    swap = give(gfull.at[mine], gfull.at[mine], 2)
    swap.wait()
    gram = gfull[...]
    row = lax.broadcasted_iota(jnp.int32, (L, L), 0)
    col = lax.broadcasted_iota(jnp.int32, (L, L), 1)
    diagonal = row == col
    total = jnp.sum(jnp.where(diagonal, gram, 0.0)) + EPSILON
    total = jnp.full((1, 1), total, jnp.float32)
    a = gram / total
    q = None
    for step in range(ITERS):
        p = jnp.where(diagonal, 1.5, 0.0) - 0.5 * a
        q = p if q is None else three_pass(p, q)
        if step < ITERS - 1:
            a = three_pass(three_pass(p, a), p)
    scale = D**0.5 * lax.rsqrt(total)
    factor = three_pass(q, term[...] * scale)

    def chunk(shift, core_of):
        index = 2 * lax.rem(coords[0] + shift, RING) + core_of
        return pl.ds(pl.multiple_of(index * COLS, COLS), COLS)

    def piece(shift, rows=slice(None)):
        return out_ref.at[rows, chunk(shift, core)]

    out_ref[:, chunk(0, core)] = factor.astype(jnp.bfloat16)
    upper, lower = pl.ds(0, HALF), pl.ds(HALF, HALF)
    right = across(piece(0), piece(0), 3, 1)
    left = across(piece(0), piece(0), 4, 3)
    gives = [give(piece(0), piece(0), 3)]
    right.wait_recv()
    on_right = across(piece(3, upper), piece(3, upper), 5, 1)
    gives.append(give(piece(3), piece(3), 4))
    left.wait_recv()
    on_left = across(piece(1, lower), piece(1, lower), 6, 3)
    gives.append(give(piece(1), piece(1), 5))
    on_right.wait_recv()
    gives.append(give(piece(2, upper), piece(2, upper), 6))
    on_left.wait_recv()
    gives.append(give(piece(2, lower), piece(2, lower), 7))
    for c in (right, left, on_right, on_left):
        c.wait_send()
    for c in gives:
        c.wait()
    for c in sent:
        c.wait_send()


def split(a):
    high = a.astype(jnp.bfloat16)
    return high, (a - high.astype(jnp.float32)).astype(jnp.bfloat16)


def mm(a, b):
    return jnp.dot(a, b, preferred_element_type=jnp.float32)


def two_pass(a, b):
    high, low = split(a)
    return mm(high, b) + mm(low, b)


def three_pass(a, b):
    ah, al = split(a)
    bh, bl = split(b)
    return mm(ah, bh) + (mm(ah, bl) + mm(al, bh))


def three_pass_nt(a, b):
    ah, al = split(a)
    bh, bl = split(b)
    return mm_nt(ah, bh) + (mm_nt(ah, bl) + mm_nt(al, bh))


def reduce_terms(partial, basis, own):
    width = QUARTER // 2
    rows = [count for _, count in PARTS]

    def buffers(lead, dims, dtype):
        return [pltpu.VMEM((*lead, *dims, r, width), dtype) for r in rows]

    def whole(dims, dtype):
        return [pltpu.VMEM((*dims, r, QUARTER), dtype) for r in rows]

    b16, f32 = jnp.bfloat16, jnp.float32
    return pl.pallas_call(
        reduce_kernel,
        out_shape=jax.ShapeDtypeStruct((L, D), jnp.bfloat16),
        in_specs=[
            pl.BlockSpec(memory_space=pl.ANY),
            pl.BlockSpec(memory_space=pl.ANY),
            pl.BlockSpec(memory_space=pltpu.VMEM),
        ],
        out_specs=pl.BlockSpec(memory_space=pltpu.VMEM),
        scratch_shapes=[
            *buffers((4,), (4, 4), b16),
            *buffers((2,), (4, 4), b16),
            *buffers((4,), (4, 4), b16),
            *whole((4, 4), b16),
            *buffers((2,), (4,), b16),
            *buffers((4,), (4,), b16),
            *whole((4,), f32),
            *buffers((2,), (), f32),
            *buffers((4,), (), f32),
            pltpu.VMEM((2, HALF, width), f32),
            pltpu.VMEM((2, 4, HALF, QUARTER), b16),
            pltpu.VMEM((L, COLS), f32),
            pltpu.VMEM((L, L), f32),
            pltpu.VMEM((HALF, L), f32),
            pltpu.VMEM((3, HALF, L), f32),
            pltpu.VMEM((L, L), f32),
            pltpu.SemaphoreType.DMA((3, 3, 6)),
            pltpu.SemaphoreType.DMA((3, 3, 6)),
            pltpu.SemaphoreType.DMA((4, 4)),
            pltpu.SemaphoreType.DMA((9,)),
            pltpu.SemaphoreType.DMA((9,)),
            pltpu.SemaphoreType.DMA((7,)),
            pltpu.SemaphoreType.DMA((7,)),
        ],
        compiler_params=pltpu.CompilerParams(
            collective_id=1, has_side_effects=True, vmem_limit_bytes=60 * 1024 * 1024
        ),
    )(partial, basis, own)


def shards(grads, block_expert, sketch):
    own = sketch[0]
    owners = block_expert[:, 0]
    theirs = lax.ppermute(owners, "dp", [(k, k ^ 1) for k in range(N_DP)])
    basis, other = gather(own, grads)
    count, slots, order = slot_table(jnp.concatenate([owners, theirs]))
    partial = local_terms(count, slots, order, basis, grads, other)
    return reduce_terms(partial, basis, own)[None]


def solution(mesh):
    in_specs = (P(("dp", "expert"), None), P(("dp", "expert"), None), P("expert", None, "dp"))
    out_specs = P("expert", None, None)
    return jax.shard_map(shards, mesh=mesh, in_specs=in_specs, out_specs=out_specs, check_vma=False)
```

```python
import functools

import jax
import jax.numpy as jnp
from jax import lax
from jax.experimental import pallas as pl
from jax.experimental.pallas import tpu as pltpu
from jax.sharding import PartitionSpec as P

D = 4096
L = 256
BLOCK = 128
NBLK = 8
EXPERTS = 16
ITERS = 5
N_DP = 8
COLS = D // N_DP
QUARTER = D // 4
HALF = L // 2
EPSILON = 1e-06
HIGHEST = lax.Precision.HIGHEST
MESH = pl.DeviceIdType.MESH
RING = 4
ORDERS = ((0, 1, 2), (1, 2, 0), (2, 0, 1))


def mm_nt(a, b):
    return lax.dot_general(a, b, (((1,), (1,)), ((), ())), preferred_element_type=jnp.float32)


def position():
    dp, expert = lax.axis_index("dp"), lax.axis_index("expert")
    return (dp // 2, expert // 4, lax.rem(expert, 4)), lax.rem(dp, 2)


def device(coords, core):
    return (2 * coords[0] + core, 4 * coords[1] + coords[2])


def moved(coords, axis, by):
    return tuple(lax.rem(c + by, RING) if k == axis else c for k, c in enumerate(coords))


def meet(coords, core):
    barrier = pltpu.get_barrier_semaphore()
    peers = [device(moved(coords, a, by), core) for a in range(3) for by in (1, 3)]
    peers.append(device(coords, 1 - core))
    for peer in peers:
        pl.semaphore_signal(barrier, inc=1, device_id=peer, device_id_type=MESH)
    pl.semaphore_wait(barrier, len(peers))


PIECES = tuple((32 * k, 32, 0, QUARTER, ORDERS[k], True) for k in range(3)) + tuple(
    (96, 32, first, count, ORDERS[k], False)
    for k, (first, count) in enumerate(((0, 384), (384, 384), (768, 256)))
)
GATHER_COPIES = 4 * sum(6 if piece[5] else 3 for piece in PIECES)
ALL = slice(None)


class GatherRing:
    def __init__(self, env, piece, fixed, axis):
        self.env, self.piece, self.fixed, self.axis = env, piece, fixed, axis
        self.ids = [env["count"] + k for k in range(4)]
        env["count"] += 4

    def view(self, shift, half=None):
        coords = self.env["coords"]
        row, rows, col, cols = self.piece[:4]
        if half is not None:
            row, rows = row + half * (rows // 2), rows // 2
        index = []
        for axis in range(3):
            step = shift if axis == self.axis else self.fixed.get(axis, 0)
            index.append(ALL if step is ALL else pl.ds(lax.rem(coords[axis] + step, RING), 1))
        return self.env["ref"].at[(*index, pl.ds(row, rows), pl.ds(col, cols))]

    def push(self, which, ref, by):
        env, k = self.env, self.ids[which]
        target = device(moved(env["coords"], self.axis, by), env["core"])
        copy = pltpu.make_async_remote_copy(
            ref, ref, env["send"].at[k], env["recv"].at[k], target, MESH
        )
        copy.start()
        env["sent"].append(copy)

    def arrived(self, which, ref):
        pltpu.make_async_copy(ref, ref, self.env["recv"].at[self.ids[which]]).wait()

    def start(self):
        self.push(0, self.view(0), 1)
        self.push(1, self.view(0), 3)

    def forward(self):
        self.arrived(0, self.view(3))
        self.push(2, self.view(3, 0), 1)
        self.arrived(1, self.view(1))
        self.push(3, self.view(1, 1), 3)

    def finish(self):
        self.arrived(2, self.view(2, 0))
        self.arrived(3, self.view(2, 1))


def gather_kernel(sketch_ref, grads_ref, basis_ref, other_ref, send, recv, pair_send, pair_recv, local):
    coords, core = position()
    meet(coords, core)
    partner = device(coords, 1 - core)
    cols = pl.ds(pl.multiple_of(core * COLS, COLS), COLS)
    own_rows = pl.ds(pl.multiple_of(core * HALF, HALF), HALF)
    other_rows = pl.ds(pl.multiple_of((1 - core) * HALF, HALF), HALF)
    spot = basis_ref.at[coords[0], coords[1], coords[2], :, cols]
    keep = pltpu.make_async_copy(sketch_ref.at[own_rows], spot, local)
    keep.start()
    give = pltpu.make_async_remote_copy(
        sketch_ref.at[other_rows], spot, pair_send.at[0], pair_recv.at[0], partner, MESH
    )
    give.start()
    swap = pltpu.make_async_remote_copy(
        grads_ref, other_ref, pair_send.at[1], pair_recv.at[1], partner, MESH
    )
    keep.wait()
    give.wait()

    env = dict(coords=coords, core=core, ref=basis_ref, send=send, recv=recv, sent=[], count=0)
    first, second, third = [], [], []
    for piece in PIECES:
        a1, a2, a3 = piece[4]
        first.append(GatherRing(env, piece, {}, a1))
        second.append(GatherRing(env, piece, {a1: ALL}, a2))
        steps = (0, 3, 1, 2) if piece[5] else (ALL,)
        third.append([GatherRing(env, piece, {a1: ALL, a2: k}, a3) for k in steps])
    sliced = [k for k, piece in enumerate(PIECES) if piece[5]]
    for ring in first:
        ring.start()
    swap.start()
    for ring in first:
        ring.forward()
    for k, ring in enumerate(first):
        ring.finish()
        second[k].start()
    for k in sliced:
        third[k][0].start()
    for ring in second:
        ring.forward()
    for k in sliced:
        third[k][1].start()
        third[k][2].start()
    for k in sliced:
        third[k][0].forward()
    for k, ring in enumerate(second):
        ring.finish()
        third[k][-1].start()
    for step in (1, 2, 3):
        for k in sliced:
            third[k][step].forward()
    for k in range(len(PIECES)):
        if k not in sliced:
            third[k][0].forward()
    for rings in third:
        for ring in rings:
            ring.finish()
    for copy in env["sent"]:
        copy.wait_send()
    swap.wait()


def gather(sketch, grads):
    return pl.pallas_call(
        gather_kernel,
        out_shape=(
            jax.ShapeDtypeStruct((4, 4, 4, HALF, QUARTER), jnp.bfloat16),
            jax.ShapeDtypeStruct(grads.shape, jnp.bfloat16),
        ),
        in_specs=[
            pl.BlockSpec(memory_space=pltpu.VMEM),
            pl.BlockSpec(memory_space=pl.ANY),
        ],
        out_specs=(pl.BlockSpec(memory_space=pl.ANY), pl.BlockSpec(memory_space=pl.ANY)),
        scratch_shapes=[
            pltpu.SemaphoreType.DMA((GATHER_COPIES,)),
            pltpu.SemaphoreType.DMA((GATHER_COPIES,)),
            pltpu.SemaphoreType.DMA((2,)),
            pltpu.SemaphoreType.DMA((2,)),
            pltpu.SemaphoreType.DMA,
        ],
        compiler_params=pltpu.CompilerParams(collective_id=0, has_side_effects=True),
    )(sketch, grads)


def slot_table(owners):
    ids = jnp.arange(EXPERTS, dtype=jnp.int32)
    hit = owners[None, :] == ids[:, None]
    count = jnp.sum(hit.astype(jnp.int32), axis=1)
    blocks = owners.shape[0]
    b = jnp.arange(blocks, dtype=jnp.int32)
    rank = jnp.sum(hit[:, None, :] & (b[None, :] < b[:, None])[None], axis=2).astype(jnp.int32)
    slot0 = jnp.sum(jnp.where(hit & (rank == 0), b[None, :], 0), axis=1)
    slots = [
        jnp.where(count > j, jnp.sum(jnp.where(hit & (rank == j), b[None, :], 0), axis=1), slot0)
        for j in range(4)
    ]
    return count, jnp.stack(slots, axis=1).reshape(-1)


class ReduceRing:
    def __init__(self, env, axis, lead, held, far, near, store):
        self.env, self.axis, self.lead = env, axis, lead
        self.held, self.far, self.near, self.store = held, far, near, store
        self.ids = [env["count"] + k for k in range(6)]
        env["count"] += 6

    def push(self, which, src, dst, by):
        env, k = self.env, self.ids[which]
        target = device(moved(env["coords"], self.axis, by), env["core"])
        copy = pltpu.make_async_remote_copy(
            src, dst, env["send"].at[k], env["recv"].at[k], target, MESH
        )
        copy.start()
        env["sent"].append(copy)

    def arrived(self, which, ref):
        pltpu.make_async_copy(ref, ref, self.env["recv"].at[self.ids[which]]).wait()

    def each(self, fn):
        if self.lead == 0:
            fn(())
            return

        def body(i, carry):
            fn((i,) if self.lead == 1 else (lax.div(i, RING), lax.rem(i, RING)))
            return carry

        lax.fori_loop(0, RING**self.lead, body, 0)

    def send_far(self):
        self.push(0, self.held(2, 0), self.far.at[0], 1)
        self.push(1, self.held(2, 1), self.far.at[1], 3)

    def send_right(self):
        self.push(2, self.held(1, 1), self.near.at[1], 1)

    def send_left(self):
        self.push(3, self.held(3, 0), self.near.at[2], 3)

    def begin(self):
        self.send_far()
        self.send_right()
        self.send_left()

    def forward_half(self, half):
        shift, dst = ((1, 0), (3, 3))[half]
        self.arrived(half, self.far.at[half])
        mine, far = self.held(shift, half), self.far

        def add(index):
            total = far[(half, *index)].astype(jnp.float32) + mine[index].astype(jnp.float32)
            far[(half, *index)] = total.astype(far.dtype)

        self.each(add)
        self.push(4 + half, far.at[half], self.near.at[dst], shift)

    def forward(self):
        self.forward_half(0)
        self.forward_half(1)

    def finish(self):
        near = self.near
        for which, slot in ((2, 1), (3, 2), (4, 0), (5, 3)):
            self.arrived(which, near.at[slot])
        for half in range(2):
            mine = self.held(0, half)

            def add(index, half=half, mine=mine):
                total = mine[index].astype(jnp.float32) + near[(half, *index)].astype(jnp.float32)
                self.store(half, index, total + near[(2 + half, *index)].astype(jnp.float32))

            self.each(add)


PARTS = ((0, 48), (48, 48), (96, 32))
AXES = ((0, 2, 1), (1, 2, 0), (2, 0, 1))
REDUCE_COPIES = 6 * (4 + 4 + 1 + 2 * 3)


def cols_of_half(half):
    return pl.ds(half * COLS, COLS)


def reduce_buffers():
    b16, f32 = jnp.bfloat16, jnp.float32
    shapes = {
        "g": pltpu.VMEM((2 * NBLK, BLOCK, D), b16),
        "s": pltpu.VMEM((2, 4, HALF, QUARTER), b16),
        "p": pltpu.VMEM((HALF, 4 * BLOCK), b16),
        "t": pltpu.VMEM((4, 4, 4, HALF, QUARTER), b16),
    }
    for k, (_, rows) in enumerate(PARTS):
        lead = (4, 4) if k == 2 else (4,)
        slices = 1 if k == 2 else 4
        shapes["far1", k] = pltpu.VMEM((slices, 2, *lead, rows, COLS), b16)
        shapes["near1", k] = pltpu.VMEM((slices, 4, *lead, rows, COLS), b16)
        shapes["far2", k] = pltpu.VMEM((2, 4, rows, COLS), b16)
        shapes["near2", k] = pltpu.VMEM((4, 4, rows, COLS), b16)
        shapes["sum2", k] = pltpu.VMEM((4, rows, QUARTER), f32)
        shapes["far3", k] = pltpu.VMEM((2, rows, COLS), f32)
        shapes["near3", k] = pltpu.VMEM((4, rows, COLS), f32)
    shapes["final"] = pltpu.VMEM((HALF, QUARTER), f32)
    shapes["whole"] = pltpu.VMEM((2, 4, HALF, QUARTER), b16)
    shapes["term"] = pltpu.VMEM((L, COLS), f32)
    shapes["gp"] = pltpu.VMEM((L, L), f32)
    shapes["gin"] = pltpu.VMEM((HALF, L), f32)
    shapes["gx"] = pltpu.VMEM((3, HALF, L), f32)
    shapes["gfull"] = pltpu.VMEM((L, L), f32)
    for name, count in (
        ("send", REDUCE_COPIES), ("recv", REDUCE_COPIES), ("load", 5),
        ("pair_send", 9), ("pair_recv", 9), ("x_send", 10), ("x_recv", 10),
    ):
        shapes[name] = pltpu.SemaphoreType.DMA((count,))
    return shapes


def reduce_kernel(
    names, count_ref, slot_ref, grads_ref, other_ref, basis_ref, sketch_ref, out_ref, *scratch
):
    buf = dict(zip(names, scratch))
    coords, core = position()
    final, whole, term, gp, gin, gx, gfull = (
        buf[k] for k in ("final", "whole", "term", "gp", "gin", "gx", "gfull")
    )
    pair_send, pair_recv, x_send, x_recv = (
        buf[k] for k in ("pair_send", "pair_recv", "x_send", "x_recv")
    )
    g_ref, s_ref, p_ref, t_ref, load = (buf[k] for k in ("g", "s", "p", "t", "load"))
    env = dict(coords=coords, core=core, send=buf["send"], recv=buf["recv"], sent=[], count=0)

    def at(axis, shift):
        return lax.rem(coords[axis] + shift, RING)

    steps = (2, 1, 3, 0)
    grads_in = [
        pltpu.make_async_copy(grads_ref, g_ref.at[0:NBLK], load.at[0]),
        pltpu.make_async_copy(other_ref, g_ref.at[NBLK : 2 * NBLK], load.at[1]),
    ]

    def basis_in(y, z, slot):
        return pltpu.make_async_copy(basis_ref.at[:, y, z], s_ref.at[slot], load.at[2 + slot])

    def compute(turn):
        step = steps[turn]
        z = at(2, step)

        def body(y, carry):
            slot = lax.rem(y, 2)
            basis_in(y, z, slot).wait()

            @pl.when(y < 3)
            def _():
                basis_in(y + 1, z, 1 - slot).start()

            e = 4 * y + z
            blocks = [slot_ref[4 * e + j] for j in range(4)]

            def rows(lo, hi):
                return jnp.concatenate([g_ref[b, :, lo:hi] for b in blocks], axis=0)

            acc = mm_nt(rows(0, QUARTER), s_ref[slot, 0])
            for x in range(1, 4):
                acc += mm_nt(rows(x * QUARTER, (x + 1) * QUARTER), s_ref[slot, x])
            place = lax.broadcasted_iota(jnp.int32, acc.shape, 0) // BLOCK
            p_ref[...] = jnp.where(place < count_ref[e], acc, 0.0).T.astype(jnp.bfloat16)
            for c in range(N_DP):
                value = mm(p_ref[...], rows(c * COLS, (c + 1) * COLS))
                t_ref[step, y, c // 2, :, (c % 2) * COLS : (c % 2 + 1) * COLS] = value.astype(
                    jnp.bfloat16
                )
            return carry

        lax.fori_loop(0, 4, body, 0)
        if turn < 3:
            basis_in(0, at(2, steps[turn + 1]), 0).start()

    def first_ring(k, slot, step):
        row, count = PARTS[k]
        rows = pl.ds(row, count)

        def held(shift, half):
            cols = cols_of_half(half)
            if k == 0:
                return t_ref.at[step, :, at(0, shift), rows, cols]
            if k == 1:
                return t_ref.at[step, at(1, shift), :, rows, cols]
            return t_ref.at[shift, :, :, rows, cols]

        def store(half, index, value):
            if k == 0:
                place = (step, index[0], coords[0])
            elif k == 1:
                place = (step, coords[1], index[0])
            else:
                place = (0, *index)
            t_ref[(*place, rows, cols_of_half(half))] = value.astype(jnp.bfloat16)

        far, near = buf["far1", k].at[slot], buf["near1", k].at[slot]
        return ReduceRing(env, k, 2 if k == 2 else 1, held, far, near, store)

    def second_ring(k):
        row, count = PARTS[k]
        rows = pl.ds(row, count)
        out = buf["sum2", k]

        def held(shift, half):
            cols = cols_of_half(half)
            if k == 0:
                return t_ref.at[shift, :, coords[0], rows, cols]
            if k == 1:
                return t_ref.at[shift, coords[1], :, rows, cols]
            return t_ref.at[0, :, at(0, shift), rows, cols]

        def store(half, index, value):
            out[(*index, ALL, cols_of_half(half))] = value

        return ReduceRing(env, AXES[k][1], 1, held, buf["far2", k], buf["near2", k], store)

    def third_ring(k):
        row, count = PARTS[k]
        axis = AXES[k][2]

        def held(shift, half):
            return buf["sum2", k].at[at(axis, shift), :, cols_of_half(half)]

        def store(half, index, value):
            final[row : row + count, half * COLS : (half + 1) * COLS] = value

        return ReduceRing(env, axis, 0, held, buf["far3", k], buf["near3", k], store)

    sliced = {
        step: [first_ring(k, slot, step) for k in range(2)] for slot, step in enumerate(steps)
    }
    deep = first_ring(2, 0, None)
    second = [second_ring(k) for k in range(3)]
    third = [third_ring(k) for k in range(3)]

    for c in grads_in:
        c.start()
    basis_in(0, at(2, steps[0]), 0).start()
    whole_own = pltpu.make_async_copy(
        basis_ref.at[:, coords[1], coords[2]], whole.at[core], load.at[4]
    )
    meet(coords, core)
    for c in grads_in:
        c.wait()

    def run(rings, method):
        for ring in rings:
            method(ring)

    begin, forward, finish = ReduceRing.begin, ReduceRing.forward, ReduceRing.finish
    compute(0)
    run(sliced[2], begin)
    deep.send_far()
    compute(1)
    run(sliced[1], begin)
    deep.send_right()
    run(sliced[2], forward)
    deep.forward_half(0)
    compute(2)
    run(sliced[3], begin)
    deep.send_left()
    deep.forward_half(1)
    run(sliced[1], forward)
    whole_own.start()
    whole_swap = pltpu.make_async_remote_copy(
        basis_ref.at[:, coords[1], coords[2]],
        whole.at[core],
        pair_send.at[8],
        pair_recv.at[8],
        device(coords, 1 - core),
        MESH,
    )
    whole_swap.start()
    run(sliced[2], finish)
    run(second[:2], ReduceRing.send_far)
    compute(3)
    run(sliced[0], begin)
    run(sliced[3], forward)
    run(sliced[1], finish)
    run(second[:2], ReduceRing.send_right)
    deep.finish()
    second[2].begin()
    run(sliced[0], forward)
    run(sliced[3], finish)
    run(second[:2], ReduceRing.send_left)
    whole_own.wait()
    whole_swap.wait()
    gp[...] = jnp.zeros_like(gp)
    for x in range(4):
        for h in range(2):
            gp[h * HALF : (h + 1) * HALF, 0:HALF] += mm_nt(whole[h, x], whole[0, x])
            gp[h * HALF : (h + 1) * HALF, HALF:] += mm_nt(whole[h, x], whole[1, x])
    run(second, forward)
    run(sliced[0], finish)
    for k in (2, 0, 1):
        second[k].finish()
        third[k].begin()
    for k in (2, 0, 1):
        third[k].forward()
    run(third, finish)
    sent = env["sent"]
    partner = device(coords, 1 - core)
    mine = pl.ds(pl.multiple_of(core * HALF, HALF), HALF)
    theirs = pl.ds(pl.multiple_of((1 - core) * HALF, HALF), HALF)

    def give(src, dst, which):
        c = pltpu.make_async_remote_copy(
            src, dst, pair_send.at[which], pair_recv.at[which], partner, MESH
        )
        c.start()
        return c

    def across(src, dst, which, by):
        c = pltpu.make_async_remote_copy(
            src, dst, x_send.at[which], x_recv.at[which], device(moved(coords, 0, by), core), MESH
        )
        c.start()
        return c

    here = pl.ds(pl.multiple_of(core * COLS, COLS), COLS)
    there = pl.ds(pl.multiple_of((1 - core) * COLS, COLS), COLS)
    swap = give(final.at[:, there], term.at[mine], 0)
    term[mine, :] = final[:, here]
    product = two_pass(gp[...], sketch_ref[...])
    swap.wait()
    average = float(BLOCK * NBLK * N_DP)
    unscaled = product + term[...] / average
    term[...] = unscaled
    gp[...] = three_pass_nt(unscaled, unscaled)
    swap = give(gp.at[theirs], gin, 1)
    swap.wait()
    gin[...] = gin[...] + gp[mine, :]
    quarter = HALF // 2
    right = across(gin, gx.at[0], 0, 1)
    left = across(gin, gx.at[1], 1, 3)
    right.wait_recv()
    on_right = across(gx.at[0, 0:quarter], gx.at[2, 0:quarter], 2, 1)
    left.wait_recv()
    on_left = across(gx.at[1, quarter:HALF], gx.at[2, quarter:HALF], 3, 3)
    for c in (right, left):
        c.wait_send()
    on_right.wait()
    on_left.wait()
    gfull[mine, :] = (gin[...] + gx[2]) + (gx[0] + gx[1])
    swap = give(gfull.at[mine], gfull.at[mine], 2)
    swap.wait()
    gram = gfull[...]
    row = lax.broadcasted_iota(jnp.int32, (L, L), 0)
    col = lax.broadcasted_iota(jnp.int32, (L, L), 1)
    diagonal = row == col
    total = jnp.sum(jnp.where(diagonal, gram, 0.0)) + EPSILON
    total = jnp.full((1, 1), total, jnp.float32)
    a = gram / total
    q = None
    for step in range(ITERS):
        p = jnp.where(diagonal, 1.5, 0.0) - 0.5 * a
        q = p if q is None else three_pass(p, q)
        if step < ITERS - 1:
            a = three_pass(three_pass(p, a), p)
    scale = D**0.5 * lax.rsqrt(total)
    factor = three_pass(q, term[...] * scale)

    def chunk(shift, core_of):
        index = 2 * lax.rem(coords[0] + shift, RING) + core_of
        return pl.ds(pl.multiple_of(index * COLS, COLS), COLS)

    def piece(shift, rows=slice(None)):
        return out_ref.at[rows, chunk(shift, core)]

    out_ref[:, chunk(0, core)] = factor.astype(jnp.bfloat16)
    upper, lower = pl.ds(0, HALF), pl.ds(HALF, HALF)
    right = across(piece(0, upper), piece(0, upper), 4, 1)
    left = across(piece(0, lower), piece(0, lower), 6, 3)
    right_rest = across(piece(0, lower), piece(0, lower), 5, 1)
    left_rest = across(piece(0, upper), piece(0, upper), 7, 3)
    gives = [give(piece(0), piece(0), 3)]
    right.wait_recv()
    on_right = across(piece(3, upper), piece(3, upper), 8, 1)
    left.wait_recv()
    on_left = across(piece(1, lower), piece(1, lower), 9, 3)
    right_rest.wait_recv()
    gives.append(give(piece(3), piece(3), 4))
    left_rest.wait_recv()
    gives.append(give(piece(1), piece(1), 5))
    on_right.wait_recv()
    gives.append(give(piece(2, upper), piece(2, upper), 6))
    on_left.wait_recv()
    gives.append(give(piece(2, lower), piece(2, lower), 7))
    for c in (right, left, right_rest, left_rest, on_right, on_left):
        c.wait_send()
    for c in gives:
        c.wait()
    for c in sent:
        c.wait_send()


def split(a):
    high = a.astype(jnp.bfloat16)
    return high, (a - high.astype(jnp.float32)).astype(jnp.bfloat16)


def mm(a, b):
    return jnp.dot(a, b, preferred_element_type=jnp.float32)


def two_pass(a, b):
    high, low = split(a)
    return mm(high, b) + mm(low, b)


def three_pass(a, b):
    ah, al = split(a)
    bh, bl = split(b)
    return mm(ah, bh) + (mm(ah, bl) + mm(al, bh))


def three_pass_nt(a, b):
    ah, al = split(a)
    bh, bl = split(b)
    return mm_nt(ah, bh) + (mm_nt(ah, bl) + mm_nt(al, bh))


def reduce_terms(count, slots, grads, other, basis, own):
    buffers = reduce_buffers()
    smem, vmem, where = (
        pl.BlockSpec(memory_space=m) for m in (pltpu.SMEM, pltpu.VMEM, pl.ANY)
    )
    return pl.pallas_call(
        functools.partial(reduce_kernel, tuple(buffers)),
        out_shape=jax.ShapeDtypeStruct((L, D), jnp.bfloat16),
        in_specs=[smem, smem, where, where, where, vmem],
        out_specs=vmem,
        scratch_shapes=list(buffers.values()),
        compiler_params=pltpu.CompilerParams(
            collective_id=1, has_side_effects=True, vmem_limit_bytes=67043328
        ),
    )(count, slots, grads, other, basis, own)


def shards(grads, block_expert, sketch):
    own = sketch[0]
    owners = block_expert[:, 0]
    theirs = lax.ppermute(owners, "dp", [(k, k ^ 1) for k in range(N_DP)])
    grads = grads.reshape(NBLK, BLOCK, D)
    basis, other = gather(own, grads)
    count, slots = slot_table(jnp.concatenate([owners, theirs]))
    return reduce_terms(count, slots, grads, other, basis, own)[None]


def solution(mesh):
    in_specs = (P(("dp", "expert"), None), P(("dp", "expert"), None), P("expert", None, "dp"))
    out_specs = P("expert", None, None)
    return jax.shard_map(shards, mesh=mesh, in_specs=in_specs, out_specs=out_specs, check_vma=False)
```

```python
import functools
import math

import jax
import jax.numpy as jnp
from jax import lax
from jax.experimental import pallas as pl
from jax.experimental.pallas import tpu as pltpu
from jax.sharding import PartitionSpec as P

D = 4096
L = 256
BLOCK = 128
NBLK = 8
EXPERTS = 16
ITERS = 5
N_DP = 8
COLS = D // N_DP
QUARTER = D // 4
HALF = L // 2
EPSILON = 1e-06
HIGHEST = lax.Precision.HIGHEST
MESH = pl.DeviceIdType.MESH
RING = 4
ORDERS = ((0, 1, 2), (1, 2, 0), (2, 0, 1))


def mm_nt(a, b):
    return lax.dot_general(a, b, (((1,), (1,)), ((), ())), preferred_element_type=jnp.float32)


def position():
    dp, expert = lax.axis_index("dp"), lax.axis_index("expert")
    return (dp // 2, expert // 4, lax.rem(expert, 4)), lax.rem(dp, 2)


def device(coords, core):
    return (2 * coords[0] + core, 4 * coords[1] + coords[2])


def moved(coords, axis, by):
    return tuple(lax.rem(c + by, RING) if k == axis else c for k, c in enumerate(coords))


def meet(coords, core):
    barrier = pltpu.get_barrier_semaphore()
    peers = [device(moved(coords, a, by), core) for a in range(3) for by in (1, 3)]
    peers.append(device(coords, 1 - core))
    for peer in peers:
        pl.semaphore_signal(barrier, inc=1, device_id=peer, device_id_type=MESH)
    pl.semaphore_wait(barrier, len(peers))


PIECES = tuple((32 * k, 32, 0, QUARTER, ORDERS[k], True) for k in range(3)) + tuple(
    (96, 32, first, count, ORDERS[k], False)
    for k, (first, count) in enumerate(((0, 384), (384, 384), (768, 256)))
)
GATHER_COPIES = 4 * sum(9 if piece[5] else 3 for piece in PIECES)
ALL = slice(None)


class GatherRing:
    def __init__(self, env, piece, fixed, axis):
        self.env, self.piece, self.fixed, self.axis = env, piece, fixed, axis
        self.ids = [env["count"] + k for k in range(4)]
        env["count"] += 4

    def view(self, shift, half=None):
        coords = self.env["coords"]
        row, rows, col, cols = self.piece[:4]
        if half is not None:
            row, rows = row + half * (rows // 2), rows // 2
        index = []
        for axis in range(3):
            step = shift if axis == self.axis else self.fixed.get(axis, 0)
            index.append(ALL if step is ALL else pl.ds(lax.rem(coords[axis] + step, RING), 1))
        return self.env["ref"].at[(*index, pl.ds(row, rows), pl.ds(col, cols))]

    def push(self, which, ref, by):
        env, k = self.env, self.ids[which]
        target = device(moved(env["coords"], self.axis, by), env["core"])
        copy = pltpu.make_async_remote_copy(
            ref, ref, env["send"].at[k], env["recv"].at[k], target, MESH
        )
        copy.start()
        env["sent"].append(copy)

    def arrived(self, which, ref):
        pltpu.make_async_copy(ref, ref, self.env["recv"].at[self.ids[which]]).wait()

    def start(self):
        self.push(0, self.view(0), 1)
        self.push(1, self.view(0), 3)

    def forward(self):
        self.arrived(0, self.view(3))
        self.push(2, self.view(3, 0), 1)
        self.arrived(1, self.view(1))
        self.push(3, self.view(1, 1), 3)

    def finish(self):
        self.arrived(2, self.view(2, 0))
        self.arrived(3, self.view(2, 1))


def gather_kernel(sketch_ref, grads_ref, basis_ref, other_ref, send, recv, pair_send, pair_recv, local):
    coords, core = position()
    meet(coords, core)
    partner = device(coords, 1 - core)
    cols = pl.ds(pl.multiple_of(core * COLS, COLS), COLS)
    own_rows = pl.ds(pl.multiple_of(core * HALF, HALF), HALF)
    other_rows = pl.ds(pl.multiple_of((1 - core) * HALF, HALF), HALF)
    spot = basis_ref.at[coords[0], coords[1], coords[2], :, cols]
    keep = pltpu.make_async_copy(sketch_ref.at[own_rows], spot, local)
    keep.start()
    give = pltpu.make_async_remote_copy(
        sketch_ref.at[other_rows], spot, pair_send.at[0], pair_recv.at[0], partner, MESH
    )
    give.start()
    swap = pltpu.make_async_remote_copy(
        grads_ref, other_ref, pair_send.at[1], pair_recv.at[1], partner, MESH
    )
    keep.wait()
    give.wait()

    env = dict(coords=coords, core=core, ref=basis_ref, send=send, recv=recv, sent=[], count=0)
    first, second, third = [], [], []
    for piece in PIECES:
        a1, a2, a3 = piece[4]
        first.append(GatherRing(env, piece, {}, a1))
        steps = (0, 3, 1, 2) if piece[5] else (ALL,)
        second.append([GatherRing(env, piece, {a1: k}, a2) for k in steps])
        third.append([GatherRing(env, piece, {a1: ALL, a2: k}, a3) for k in steps])
    sliced = [k for k, piece in enumerate(PIECES) if piece[5]]
    for ring in first:
        ring.start()
    for k in sliced:
        second[k][0].start()
    swap.start()
    for k, ring in enumerate(first):
        ring.forward()
        if k in sliced:
            second[k][1].start()
            second[k][2].start()
    for k in sliced:
        second[k][0].forward()
    for k, ring in enumerate(first):
        ring.finish()
        second[k][-1].start()
    for k in sliced:
        third[k][0].start()
    for step in (1, 2):
        for k in sliced:
            second[k][step].forward()
    for rings in second:
        rings[-1].forward()
    for k in sliced:
        third[k][1].start()
        third[k][2].start()
    for k in sliced:
        third[k][0].forward()
    for k, rings in enumerate(second):
        for ring in rings:
            ring.finish()
        third[k][-1].start()
    for step in (1, 2, 3):
        for k in sliced:
            third[k][step].forward()
    for k in range(len(PIECES)):
        if k not in sliced:
            third[k][0].forward()
    for rings in third:
        for ring in rings:
            ring.finish()
    for copy in env["sent"]:
        copy.wait_send()
    swap.wait()


def gather(sketch, grads):
    return pl.pallas_call(
        gather_kernel,
        out_shape=(
            jax.ShapeDtypeStruct((4, 4, 4, HALF, QUARTER), jnp.bfloat16),
            jax.ShapeDtypeStruct(grads.shape, jnp.bfloat16),
        ),
        in_specs=[
            pl.BlockSpec(memory_space=pltpu.VMEM),
            pl.BlockSpec(memory_space=pl.ANY),
        ],
        out_specs=(pl.BlockSpec(memory_space=pl.ANY), pl.BlockSpec(memory_space=pl.ANY)),
        scratch_shapes=[
            pltpu.SemaphoreType.DMA((GATHER_COPIES,)),
            pltpu.SemaphoreType.DMA((GATHER_COPIES,)),
            pltpu.SemaphoreType.DMA((2,)),
            pltpu.SemaphoreType.DMA((2,)),
            pltpu.SemaphoreType.DMA,
        ],
        compiler_params=pltpu.CompilerParams(collective_id=0, has_side_effects=True),
    )(sketch, grads)


def slot_table(owners):
    ids = jnp.arange(EXPERTS, dtype=jnp.int32)
    hit = owners[None, :] == ids[:, None]
    count = jnp.sum(hit.astype(jnp.int32), axis=1)
    blocks = owners.shape[0]
    b = jnp.arange(blocks, dtype=jnp.int32)
    rank = jnp.sum(hit[:, None, :] & (b[None, :] < b[:, None])[None], axis=2).astype(jnp.int32)
    slot0 = jnp.sum(jnp.where(hit & (rank == 0), b[None, :], 0), axis=1)
    slots = [
        jnp.where(count > j, jnp.sum(jnp.where(hit & (rank == j), b[None, :], 0), axis=1), slot0)
        for j in range(4)
    ]
    return count, jnp.stack(slots, axis=1).reshape(-1)


class ReduceRing:
    def __init__(self, env, axis, lead, held, far, near, store):
        self.env, self.axis, self.lead = env, axis, lead
        self.held, self.far, self.near, self.store = held, far, near, store
        self.ids = [env["count"] + k for k in range(6)]
        env["count"] += 6

    def push(self, which, src, dst, by):
        env, k = self.env, self.ids[which]
        target = device(moved(env["coords"], self.axis, by), env["core"])
        copy = pltpu.make_async_remote_copy(
            src, dst, env["send"].at[k], env["recv"].at[k], target, MESH
        )
        copy.start()
        env["sent"].append(copy)

    def arrived(self, which, ref):
        pltpu.make_async_copy(ref, ref, self.env["recv"].at[self.ids[which]]).wait()

    def each(self, fn):
        if not self.lead:
            fn(())
            return

        def body(i, carry):
            fn((i,) if len(self.lead) == 1 else (lax.div(i, RING), lax.rem(i, RING)))
            return carry

        lax.fori_loop(0, math.prod(self.lead), body, 0)

    def send_far(self):
        self.push(0, self.held(2, 0), self.far.at[0], 1)
        self.push(1, self.held(2, 1), self.far.at[1], 3)

    def send_right(self):
        self.push(2, self.held(1, 1), self.near.at[1], 1)

    def send_left(self):
        self.push(3, self.held(3, 0), self.near.at[2], 3)

    def begin(self):
        self.send_far()
        self.send_right()
        self.send_left()

    def forward_half(self, half):
        shift, dst = ((1, 0), (3, 3))[half]
        self.arrived(half, self.far.at[half])
        mine, far = self.held(shift, half), self.far

        def add(index):
            total = far[(half, *index)].astype(jnp.float32) + mine[index].astype(jnp.float32)
            far[(half, *index)] = total.astype(far.dtype)

        self.each(add)
        self.push(4 + half, far.at[half], self.near.at[dst], shift)

    def forward(self):
        self.forward_half(0)
        self.forward_half(1)

    def finish(self):
        near = self.near
        for which, slot in ((2, 1), (3, 2), (4, 0), (5, 3)):
            self.arrived(which, near.at[slot])
        for half in range(2):
            mine = self.held(0, half)

            def add(index, half=half, mine=mine):
                total = mine[index].astype(jnp.float32) + near[(half, *index)].astype(jnp.float32)
                self.store(half, index, total + near[(2 + half, *index)].astype(jnp.float32))

            self.each(add)


PARTS = ((0, 48), (48, 48), (96, 32))
AXES = ((0, 2, 1), (1, 2, 0), (2, 0, 1))
REDUCE_COPIES = 6 * (8 + 4 + 2 + 2 * 3)
STEPS = (2, 1, 3, 0)
PLACE = {2: 0, 1: 1, 3: 2, 0: 3}


def cols_of_half(half):
    return pl.ds(half * COLS, COLS)


def reduce_buffers():
    b16, f32 = jnp.bfloat16, jnp.float32
    shapes = {
        "g": pltpu.VMEM((2 * NBLK, BLOCK, D), b16),
        "s": pltpu.VMEM((2, 4, HALF, QUARTER), b16),
        "p": pltpu.VMEM((HALF, 4 * BLOCK), b16),
        "t": pltpu.VMEM((4, 4, 4, HALF, QUARTER), b16),
    }
    for k, (_, rows) in enumerate(PARTS):
        slices, lead = ((8, (2,)), (4, (4,)), (2, (2, 4)))[k]
        shapes["far1", k] = pltpu.VMEM((slices, 2, *lead, rows, COLS), b16)
        shapes["near1", k] = pltpu.VMEM((slices, 4, *lead, rows, COLS), b16)
        shapes["far2", k] = pltpu.VMEM((2, 4, rows, COLS), b16)
        shapes["near2", k] = pltpu.VMEM((4, 4, rows, COLS), b16)
        shapes["sum2", k] = pltpu.VMEM((4, rows, QUARTER), f32)
        shapes["far3", k] = pltpu.VMEM((2, rows, COLS), f32)
        shapes["near3", k] = pltpu.VMEM((4, rows, COLS), f32)
    shapes["final"] = pltpu.VMEM((HALF, QUARTER), f32)
    shapes["whole"] = pltpu.VMEM((2, 4, HALF, QUARTER), b16)
    shapes["term"] = pltpu.VMEM((L, COLS), f32)
    shapes["gp"] = pltpu.VMEM((L, L), f32)
    shapes["gin"] = pltpu.VMEM((HALF, L), f32)
    shapes["gx"] = pltpu.VMEM((3, HALF, L), f32)
    shapes["gfull"] = pltpu.VMEM((L, L), f32)
    for name, count in (
        ("send", REDUCE_COPIES), ("recv", REDUCE_COPIES), ("load", 5),
        ("pair_send", 9), ("pair_recv", 9), ("x_send", 10), ("x_recv", 10),
    ):
        shapes[name] = pltpu.SemaphoreType.DMA((count,))
    return shapes


def reduce_kernel(
    names, count_ref, slot_ref, grads_ref, other_ref, basis_ref, sketch_ref, out_ref, *scratch
):
    buf = dict(zip(names, scratch))
    coords, core = position()
    final, whole, term, gp, gin, gx, gfull = (
        buf[k] for k in ("final", "whole", "term", "gp", "gin", "gx", "gfull")
    )
    pair_send, pair_recv, x_send, x_recv = (
        buf[k] for k in ("pair_send", "pair_recv", "x_send", "x_recv")
    )
    g_ref, s_ref, p_ref, t_ref, load = (buf[k] for k in ("g", "s", "p", "t", "load"))
    env = dict(coords=coords, core=core, send=buf["send"], recv=buf["recv"], sent=[], count=0)

    def at(axis, shift):
        return lax.rem(coords[axis] + shift, RING)

    grads_in = [
        pltpu.make_async_copy(grads_ref, g_ref.at[0:NBLK], load.at[0]),
        pltpu.make_async_copy(other_ref, g_ref.at[NBLK : 2 * NBLK], load.at[1]),
    ]

    def basis_in(y, z, slot):
        return pltpu.make_async_copy(basis_ref.at[:, y, z], s_ref.at[slot], load.at[2 + slot])

    def compute(turn, part):
        step = STEPS[turn]
        z = at(2, step)
        shifts = STEPS[2 * part : 2 * part + 2]

        def body(i, carry):
            y = lax.rem(coords[1] + shifts[0] + i * (shifts[1] - shifts[0]), RING)
            basis_in(y, z, i).wait()

            @pl.when(i == 0)
            def _():
                basis_in(at(1, shifts[1]), z, 1).start()

            if turn < 3 or part == 0:
                z_next = z if part == 0 else at(2, STEPS[turn + 1])

                @pl.when(i == 1)
                def _():
                    basis_in(at(1, STEPS[2 - 2 * part]), z_next, 0).start()

            e = 4 * y + z
            blocks = [slot_ref[4 * e + j] for j in range(4)]

            def rows(lo, hi):
                return jnp.concatenate([g_ref[b, :, lo:hi] for b in blocks], axis=0)

            acc = mm_nt(rows(0, QUARTER), s_ref[i, 0])
            for x in range(1, 4):
                acc += mm_nt(rows(x * QUARTER, (x + 1) * QUARTER), s_ref[i, x])
            place = lax.broadcasted_iota(jnp.int32, acc.shape, 0) // BLOCK
            p_ref[...] = jnp.where(place < count_ref[e], acc, 0.0).T.astype(jnp.bfloat16)
            for c in range(N_DP):
                value = mm(p_ref[...], rows(c * COLS, (c + 1) * COLS))
                cols = slice((c % 2) * COLS, (c % 2 + 1) * COLS)
                t_ref[step, 2 * part + i, c // 2, :, cols] = value.astype(jnp.bfloat16)
            return carry

        lax.fori_loop(0, 2, body, 0)

    def first_ring(k, slot, step, part):
        row, count = PARTS[k]
        rows = pl.ds(row, count)
        base = 2 * part

        def held(shift, half):
            cols = cols_of_half(half)
            if k == 0:
                return t_ref.at[step, base : base + 2, at(0, shift), rows, cols]
            if k == 1:
                return t_ref.at[step, PLACE[shift], :, rows, cols]
            return t_ref.at[shift, base : base + 2, :, rows, cols]

        def store(half, index, value):
            if k == 0:
                place = (step, base + index[0], coords[0])
            elif k == 1:
                place = (step, PLACE[0], index[0])
            else:
                place = (0, base + index[0], index[1])
            t_ref[(*place, rows, cols_of_half(half))] = value.astype(jnp.bfloat16)

        far, near = buf["far1", k].at[slot], buf["near1", k].at[slot]
        return ReduceRing(env, k, ((2,), (4,), (2, 4))[k], held, far, near, store)

    def second_ring(k):
        row, count = PARTS[k]
        rows = pl.ds(row, count)
        out = buf["sum2", k]

        def held(shift, half):
            cols = cols_of_half(half)
            if k == 0:
                return t_ref.at[shift, :, coords[0], rows, cols]
            if k == 1:
                return t_ref.at[shift, PLACE[0], :, rows, cols]
            return t_ref.at[0, :, at(0, shift), rows, cols]

        def store(half, index, value):
            out[(*index, ALL, cols_of_half(half))] = value

        return ReduceRing(env, AXES[k][1], (4,), held, buf["far2", k], buf["near2", k], store)

    def third_ring(k):
        row, count = PARTS[k]
        axis = AXES[k][2]

        def held(shift, half):
            place = PLACE[shift] if axis == 1 else at(axis, shift)
            return buf["sum2", k].at[place, :, cols_of_half(half)]

        def store(half, index, value):
            final[row : row + count, half * COLS : (half + 1) * COLS] = value

        return ReduceRing(env, axis, (), held, buf["far3", k], buf["near3", k], store)

    xs = [[first_ring(0, 2 * t + h, STEPS[t], h) for h in range(2)] for t in range(4)]
    ys = [first_ring(1, t, STEPS[t], 0) for t in range(4)]
    zs = [first_ring(2, h, None, h) for h in range(2)]
    second = [second_ring(k) for k in range(3)]
    third = [third_ring(k) for k in range(3)]

    for c in grads_in:
        c.start()
    basis_in(at(1, STEPS[0]), at(2, STEPS[0]), 0).start()
    whole_own = pltpu.make_async_copy(
        basis_ref.at[:, coords[1], coords[2]], whole.at[core], load.at[4]
    )
    meet(coords, core)
    for c in grads_in:
        c.wait()

    def run(rings, method):
        for ring in rings:
            method(ring)

    def batch(turn, part):
        compute(turn, part)
        xs[turn][part].begin()
        if part == 0:
            ys[turn].send_far()
            ys[turn].send_right()
        else:
            ys[turn].send_left()
        if turn < 3:
            (ReduceRing.send_far, ReduceRing.send_right, ReduceRing.send_left)[turn](zs[part])

    forward, finish = ReduceRing.forward, ReduceRing.finish
    batch(0, 0)
    batch(0, 1)
    batch(1, 0)
    xs[0][0].forward()
    batch(1, 1)
    xs[0][1].forward()
    ys[0].forward()
    zs[0].forward_half(0)
    batch(2, 0)
    zs[1].forward_half(0)
    xs[1][0].forward()
    whole_own.start()
    whole_swap = pltpu.make_async_remote_copy(
        basis_ref.at[:, coords[1], coords[2]],
        whole.at[core],
        pair_send.at[8],
        pair_recv.at[8],
        device(coords, 1 - core),
        MESH,
    )
    whole_swap.start()
    batch(2, 1)
    zs[0].forward_half(1)
    xs[1][1].forward()
    ys[1].forward()
    run(xs[0], finish)
    ys[0].finish()
    run(second[:2], ReduceRing.send_far)
    batch(3, 0)
    zs[1].forward_half(1)
    xs[2][0].forward()
    batch(3, 1)
    xs[2][1].forward()
    ys[2].forward()
    run(xs[1], finish)
    ys[1].finish()
    run(second[:2], ReduceRing.send_right)
    run(xs[3], forward)
    ys[3].forward()
    run(zs, finish)
    second[2].begin()
    run(xs[2], finish)
    ys[2].finish()
    run(second[:2], ReduceRing.send_left)
    whole_own.wait()
    whole_swap.wait()
    gp[...] = jnp.zeros_like(gp)
    for x in range(4):
        for h in range(2):
            gp[h * HALF : (h + 1) * HALF, 0:HALF] += mm_nt(whole[h, x], whole[0, x])
            gp[h * HALF : (h + 1) * HALF, HALF:] += mm_nt(whole[h, x], whole[1, x])
    run(second, forward)
    run(xs[3], finish)
    ys[3].finish()
    for k in (2, 0, 1):
        second[k].finish()
        third[k].begin()
    for k in (2, 0, 1):
        third[k].forward()
    run(third, finish)
    sent = env["sent"]
    partner = device(coords, 1 - core)
    mine = pl.ds(pl.multiple_of(core * HALF, HALF), HALF)
    theirs = pl.ds(pl.multiple_of((1 - core) * HALF, HALF), HALF)

    def give(src, dst, which):
        c = pltpu.make_async_remote_copy(
            src, dst, pair_send.at[which], pair_recv.at[which], partner, MESH
        )
        c.start()
        return c

    def across(src, dst, which, by):
        c = pltpu.make_async_remote_copy(
            src, dst, x_send.at[which], x_recv.at[which], device(moved(coords, 0, by), core), MESH
        )
        c.start()
        return c

    here = pl.ds(pl.multiple_of(core * COLS, COLS), COLS)
    there = pl.ds(pl.multiple_of((1 - core) * COLS, COLS), COLS)
    swap = give(final.at[:, there], term.at[mine], 0)
    term[mine, :] = final[:, here]
    product = two_pass(gp[...], sketch_ref[...])
    swap.wait()
    average = float(BLOCK * NBLK * N_DP)
    unscaled = product + term[...] / average
    term[...] = unscaled
    gp[...] = three_pass_nt(unscaled, unscaled)
    swap = give(gp.at[theirs], gin, 1)
    swap.wait()
    gin[...] = gin[...] + gp[mine, :]
    quarter = HALF // 2
    right = across(gin, gx.at[0], 0, 1)
    left = across(gin, gx.at[1], 1, 3)
    right.wait_recv()
    on_right = across(gx.at[0, 0:quarter], gx.at[2, 0:quarter], 2, 1)
    left.wait_recv()
    on_left = across(gx.at[1, quarter:HALF], gx.at[2, quarter:HALF], 3, 3)
    for c in (right, left):
        c.wait_send()
    on_right.wait()
    on_left.wait()
    gfull[mine, :] = (gin[...] + gx[2]) + (gx[0] + gx[1])
    swap = give(gfull.at[mine], gfull.at[mine], 2)
    swap.wait()
    gram = gfull[...]
    row = lax.broadcasted_iota(jnp.int32, (L, L), 0)
    col = lax.broadcasted_iota(jnp.int32, (L, L), 1)
    diagonal = row == col
    total = jnp.sum(jnp.where(diagonal, gram, 0.0)) + EPSILON
    total = jnp.full((1, 1), total, jnp.float32)
    a = gram / total
    q = None
    for step in range(ITERS):
        p = jnp.where(diagonal, 1.5, 0.0) - 0.5 * a
        q = p if q is None else three_pass(p, q)
        if step < ITERS - 1:
            a = three_pass(three_pass(p, a), p)
    scale = D**0.5 * lax.rsqrt(total)
    factor = three_pass(q, term[...] * scale)

    def chunk(shift, core_of):
        index = 2 * lax.rem(coords[0] + shift, RING) + core_of
        return pl.ds(pl.multiple_of(index * COLS, COLS), COLS)

    def piece(shift, rows=slice(None)):
        return out_ref.at[rows, chunk(shift, core)]

    out_ref[:, chunk(0, core)] = factor.astype(jnp.bfloat16)
    upper, lower = pl.ds(0, HALF), pl.ds(HALF, HALF)
    right = across(piece(0, upper), piece(0, upper), 4, 1)
    left = across(piece(0, lower), piece(0, lower), 6, 3)
    right_rest = across(piece(0, lower), piece(0, lower), 5, 1)
    left_rest = across(piece(0, upper), piece(0, upper), 7, 3)
    gives = [give(piece(0), piece(0), 3)]
    right.wait_recv()
    on_right = across(piece(3, upper), piece(3, upper), 8, 1)
    left.wait_recv()
    on_left = across(piece(1, lower), piece(1, lower), 9, 3)
    right_rest.wait_recv()
    gives.append(give(piece(3), piece(3), 4))
    left_rest.wait_recv()
    gives.append(give(piece(1), piece(1), 5))
    on_right.wait_recv()
    gives.append(give(piece(2, upper), piece(2, upper), 6))
    on_left.wait_recv()
    gives.append(give(piece(2, lower), piece(2, lower), 7))
    for c in (right, left, right_rest, left_rest, on_right, on_left):
        c.wait_send()
    for c in gives:
        c.wait()
    for c in sent:
        c.wait_send()


def split(a):
    high = a.astype(jnp.bfloat16)
    return high, (a - high.astype(jnp.float32)).astype(jnp.bfloat16)


def mm(a, b):
    return jnp.dot(a, b, preferred_element_type=jnp.float32)


def two_pass(a, b):
    high, low = split(a)
    return mm(high, b) + mm(low, b)


def three_pass(a, b):
    ah, al = split(a)
    bh, bl = split(b)
    return mm(ah, bh) + (mm(ah, bl) + mm(al, bh))


def three_pass_nt(a, b):
    ah, al = split(a)
    bh, bl = split(b)
    return mm_nt(ah, bh) + (mm_nt(ah, bl) + mm_nt(al, bh))


def reduce_terms(count, slots, grads, other, basis, own):
    buffers = reduce_buffers()
    smem, vmem, where = (
        pl.BlockSpec(memory_space=m) for m in (pltpu.SMEM, pltpu.VMEM, pl.ANY)
    )
    return pl.pallas_call(
        functools.partial(reduce_kernel, tuple(buffers)),
        out_shape=jax.ShapeDtypeStruct((L, D), jnp.bfloat16),
        in_specs=[smem, smem, where, where, where, vmem],
        out_specs=vmem,
        scratch_shapes=list(buffers.values()),
        compiler_params=pltpu.CompilerParams(
            collective_id=1, has_side_effects=True, vmem_limit_bytes=67043328
        ),
    )(count, slots, grads, other, basis, own)


def shards(grads, block_expert, sketch):
    own = sketch[0]
    owners = block_expert[:, 0]
    theirs = lax.ppermute(owners, "dp", [(k, k ^ 1) for k in range(N_DP)])
    grads = grads.reshape(NBLK, BLOCK, D)
    basis, other = gather(own, grads)
    count, slots = slot_table(jnp.concatenate([owners, theirs]))
    return reduce_terms(count, slots, grads, other, basis, own)[None]


def solution(mesh):
    in_specs = (P(("dp", "expert"), None), P(("dp", "expert"), None), P("expert", None, "dp"))
    out_specs = P("expert", None, None)
    return jax.shard_map(shards, mesh=mesh, in_specs=in_specs, out_specs=out_specs, check_vma=False)
```

```python
import functools
import math

import jax
import jax.numpy as jnp
from jax import lax
from jax.experimental import pallas as pl
from jax.experimental.pallas import tpu as pltpu
from jax.sharding import PartitionSpec as P

D = 4096
L = 256
BLOCK = 128
NBLK = 8
EXPERTS = 16
ITERS = 5
N_DP = 8
COLS = D // N_DP
QUARTER = D // 4
HALF = L // 2
EPSILON = 1e-06
HIGHEST = lax.Precision.HIGHEST
MESH = pl.DeviceIdType.MESH
RING = 4
ORDERS = ((0, 1, 2), (1, 2, 0), (2, 0, 1))


def mm_nt(a, b):
    return lax.dot_general(a, b, (((1,), (1,)), ((), ())), preferred_element_type=jnp.float32)


def position():
    dp, expert = lax.axis_index("dp"), lax.axis_index("expert")
    return (dp // 2, expert // 4, lax.rem(expert, 4)), lax.rem(dp, 2)


def device(coords, core):
    return (2 * coords[0] + core, 4 * coords[1] + coords[2])


def moved(coords, axis, by):
    return tuple(lax.rem(c + by, RING) if k == axis else c for k, c in enumerate(coords))


def meet(coords, core):
    barrier = pltpu.get_barrier_semaphore()
    peers = [device(moved(coords, a, by), core) for a in range(3) for by in (1, 3)]
    peers.append(device(coords, 1 - core))
    for peer in peers:
        pl.semaphore_signal(barrier, inc=1, device_id=peer, device_id_type=MESH)
    pl.semaphore_wait(barrier, len(peers))


PIECES = tuple((32 * k, 32, 0, QUARTER, ORDERS[k], True) for k in range(3)) + tuple(
    (96, 32, first, count, ORDERS[k], False)
    for k, (first, count) in enumerate(((0, 384), (384, 384), (768, 256)))
)
GATHER_COPIES = 4 * sum(9 if piece[5] else 3 for piece in PIECES)
ALL = slice(None)


class GatherRing:
    def __init__(self, env, piece, fixed, axis):
        self.env, self.piece, self.fixed, self.axis = env, piece, fixed, axis
        self.ids = [env["count"] + k for k in range(4)]
        env["count"] += 4

    def view(self, shift, half=None):
        coords = self.env["coords"]
        row, rows, col, cols = self.piece[:4]
        if half is not None:
            row, rows = row + half * (rows // 2), rows // 2
        index = []
        for axis in range(3):
            step = shift if axis == self.axis else self.fixed.get(axis, 0)
            index.append(ALL if step is ALL else pl.ds(lax.rem(coords[axis] + step, RING), 1))
        return self.env["ref"].at[(*index, pl.ds(row, rows), pl.ds(col, cols))]

    def push(self, which, ref, by):
        env, k = self.env, self.ids[which]
        target = device(moved(env["coords"], self.axis, by), env["core"])
        copy = pltpu.make_async_remote_copy(
            ref, ref, env["send"].at[k], env["recv"].at[k], target, MESH
        )
        copy.start()
        env["sent"].append(copy)

    def arrived(self, which, ref):
        pltpu.make_async_copy(ref, ref, self.env["recv"].at[self.ids[which]]).wait()

    def start(self):
        self.push(0, self.view(0), 1)
        self.push(1, self.view(0), 3)

    def forward(self):
        self.arrived(0, self.view(3))
        self.push(2, self.view(3, 0), 1)
        self.arrived(1, self.view(1))
        self.push(3, self.view(1, 1), 3)

    def finish(self):
        self.arrived(2, self.view(2, 0))
        self.arrived(3, self.view(2, 1))


def gather_kernel(sketch_ref, grads_ref, basis_ref, other_ref, send, recv, pair_send, pair_recv, local):
    coords, core = position()
    meet(coords, core)
    partner = device(coords, 1 - core)
    cols = pl.ds(pl.multiple_of(core * COLS, COLS), COLS)
    own_rows = pl.ds(pl.multiple_of(core * HALF, HALF), HALF)
    other_rows = pl.ds(pl.multiple_of((1 - core) * HALF, HALF), HALF)
    spot = basis_ref.at[coords[0], coords[1], coords[2], :, cols]
    keep = pltpu.make_async_copy(sketch_ref.at[own_rows], spot, local)
    keep.start()
    give = pltpu.make_async_remote_copy(
        sketch_ref.at[other_rows], spot, pair_send.at[0], pair_recv.at[0], partner, MESH
    )
    give.start()
    swap = pltpu.make_async_remote_copy(
        grads_ref, other_ref, pair_send.at[1], pair_recv.at[1], partner, MESH
    )
    keep.wait()
    give.wait()

    env = dict(coords=coords, core=core, ref=basis_ref, send=send, recv=recv, sent=[], count=0)
    first, second, third = [], [], []
    for piece in PIECES:
        a1, a2, a3 = piece[4]
        first.append(GatherRing(env, piece, {}, a1))
        steps = (0, 3, 1, 2) if piece[5] else (ALL,)
        second.append([GatherRing(env, piece, {a1: k}, a2) for k in steps])
        third.append([GatherRing(env, piece, {a1: ALL, a2: k}, a3) for k in steps])
    sliced = [k for k, piece in enumerate(PIECES) if piece[5]]
    for ring in first:
        ring.start()
    for k in sliced:
        second[k][0].start()
    swap.start()
    for k, ring in enumerate(first):
        ring.forward()
        if k in sliced:
            second[k][1].start()
            second[k][2].start()
    for k in sliced:
        second[k][0].forward()
    for k, ring in enumerate(first):
        ring.finish()
        second[k][-1].start()
    for k in sliced:
        third[k][0].start()
    for step in (1, 2):
        for k in sliced:
            second[k][step].forward()
    for rings in second:
        rings[-1].forward()
    for k in sliced:
        third[k][1].start()
        third[k][2].start()
    for k in sliced:
        third[k][0].forward()
    for k, rings in enumerate(second):
        for ring in rings:
            ring.finish()
        third[k][-1].start()
    for step in (1, 2, 3):
        for k in sliced:
            third[k][step].forward()
    for k in range(len(PIECES)):
        if k not in sliced:
            third[k][0].forward()
    for rings in third:
        for ring in rings:
            ring.finish()
    for copy in env["sent"]:
        copy.wait_send()
    swap.wait()


def gather(sketch, grads):
    return pl.pallas_call(
        gather_kernel,
        out_shape=(
            jax.ShapeDtypeStruct((4, 4, 4, HALF, QUARTER), jnp.bfloat16),
            jax.ShapeDtypeStruct(grads.shape, jnp.bfloat16),
        ),
        in_specs=[
            pl.BlockSpec(memory_space=pltpu.VMEM),
            pl.BlockSpec(memory_space=pl.ANY),
        ],
        out_specs=(pl.BlockSpec(memory_space=pl.ANY), pl.BlockSpec(memory_space=pl.ANY)),
        scratch_shapes=[
            pltpu.SemaphoreType.DMA((GATHER_COPIES,)),
            pltpu.SemaphoreType.DMA((GATHER_COPIES,)),
            pltpu.SemaphoreType.DMA((2,)),
            pltpu.SemaphoreType.DMA((2,)),
            pltpu.SemaphoreType.DMA,
        ],
        compiler_params=pltpu.CompilerParams(collective_id=0, has_side_effects=True),
    )(sketch, grads)


def slot_table(owners):
    ids = jnp.arange(EXPERTS, dtype=jnp.int32)
    hit = owners[None, :] == ids[:, None]
    count = jnp.sum(hit.astype(jnp.int32), axis=1)
    blocks = owners.shape[0]
    b = jnp.arange(blocks, dtype=jnp.int32)
    rank = jnp.sum(hit[:, None, :] & (b[None, :] < b[:, None])[None], axis=2).astype(jnp.int32)
    slot0 = jnp.sum(jnp.where(hit & (rank == 0), b[None, :], 0), axis=1)
    slots = [
        jnp.where(count > j, jnp.sum(jnp.where(hit & (rank == j), b[None, :], 0), axis=1), slot0)
        for j in range(4)
    ]
    return count, jnp.stack(slots, axis=1).reshape(-1)


class ReduceRing:
    def __init__(self, env, axis, lead, held, far, near, store):
        self.env, self.axis, self.lead = env, axis, lead
        self.held, self.far, self.near, self.store = held, far, near, store
        self.ids = [env["count"] + k for k in range(6)]
        env["count"] += 6

    def push(self, which, src, dst, by):
        env, k = self.env, self.ids[which]
        target = device(moved(env["coords"], self.axis, by), env["core"])
        copy = pltpu.make_async_remote_copy(
            src, dst, env["send"].at[k], env["recv"].at[k], target, MESH
        )
        copy.start()
        env["sent"].append(copy)

    def arrived(self, which, ref):
        pltpu.make_async_copy(ref, ref, self.env["recv"].at[self.ids[which]]).wait()

    def each(self, fn):
        if not self.lead:
            fn(())
            return

        def body(i, carry):
            fn((i,) if len(self.lead) == 1 else (lax.div(i, RING), lax.rem(i, RING)))
            return carry

        lax.fori_loop(0, math.prod(self.lead), body, 0)

    def send_far(self):
        self.push(0, self.held(2, 0), self.far.at[0], 1)
        self.push(1, self.held(2, 1), self.far.at[1], 3)

    def send_right(self):
        self.push(2, self.held(1, 1), self.near.at[1], 1)

    def send_left(self):
        self.push(3, self.held(3, 0), self.near.at[2], 3)

    def begin(self):
        self.send_far()
        self.send_right()
        self.send_left()

    def forward_half(self, half):
        shift, dst = ((1, 0), (3, 3))[half]
        self.arrived(half, self.far.at[half])
        mine, far = self.held(shift, half), self.far

        def add(index):
            total = far[(half, *index)].astype(jnp.float32) + mine[index].astype(jnp.float32)
            far[(half, *index)] = total.astype(far.dtype)

        self.each(add)
        self.push(4 + half, far.at[half], self.near.at[dst], shift)

    def forward(self):
        self.forward_half(0)
        self.forward_half(1)

    def finish(self):
        near = self.near
        for which, slot in ((2, 1), (3, 2), (4, 0), (5, 3)):
            self.arrived(which, near.at[slot])
        for half in range(2):
            mine = self.held(0, half)

            def add(index, half=half, mine=mine):
                total = mine[index].astype(jnp.float32) + near[(half, *index)].astype(jnp.float32)
                self.store(half, index, total + near[(2 + half, *index)].astype(jnp.float32))

            self.each(add)


PARTS = ((0, 48), (48, 48), (96, 32))
AXES = ((0, 2, 1), (1, 2, 0), (2, 0, 1))
REDUCE_COPIES = 6 * (8 + 4 + 2 + 2 * 3)
STEPS = (2, 1, 3, 0)
PLACE = {2: 0, 1: 1, 3: 2, 0: 3}


def cols_of_half(half):
    return pl.ds(half * COLS, COLS)


def reduce_buffers():
    b16, f32 = jnp.bfloat16, jnp.float32
    shapes = {
        "g": pltpu.VMEM((2 * NBLK, BLOCK, D), b16),
        "s": pltpu.VMEM((2, 4, HALF, QUARTER), b16),
        "p": pltpu.VMEM((HALF, 4 * BLOCK), b16),
        "t": pltpu.VMEM((4, 4, 4, HALF, QUARTER), b16),
    }
    for k, (_, rows) in enumerate(PARTS):
        slices, lead = ((8, (2,)), (4, (4,)), (2, (2, 4)))[k]
        shapes["far1", k] = pltpu.VMEM((slices, 2, *lead, rows, COLS), b16)
        shapes["near1", k] = pltpu.VMEM((slices, 4, *lead, rows, COLS), b16)
        shapes["far2", k] = pltpu.VMEM((2, 4, rows, COLS), b16)
        shapes["near2", k] = pltpu.VMEM((4, 4, rows, COLS), b16)
        shapes["sum2", k] = pltpu.VMEM((4, rows, QUARTER), f32)
        shapes["far3", k] = pltpu.VMEM((2, rows, COLS), f32)
        shapes["near3", k] = pltpu.VMEM((4, rows, COLS), f32)
    shapes["final"] = pltpu.VMEM((HALF, QUARTER), f32)
    shapes["whole"] = pltpu.VMEM((2, 4, HALF, QUARTER), b16)
    shapes["term"] = pltpu.VMEM((L, COLS), f32)
    shapes["gp"] = pltpu.VMEM((L, L), f32)
    shapes["gin"] = pltpu.VMEM((HALF, L), f32)
    shapes["gx"] = pltpu.VMEM((3, HALF, L), f32)
    shapes["gfull"] = pltpu.VMEM((L, L), f32)
    for name, count in (
        ("send", REDUCE_COPIES), ("recv", REDUCE_COPIES), ("load", 5),
        ("pair_send", 9), ("pair_recv", 9), ("x_send", 12), ("x_recv", 12),
    ):
        shapes[name] = pltpu.SemaphoreType.DMA((count,))
    return shapes


def reduce_kernel(
    names, count_ref, slot_ref, grads_ref, other_ref, basis_ref, sketch_ref, out_ref, *scratch
):
    buf = dict(zip(names, scratch))
    coords, core = position()
    final, whole, term, gp, gin, gx, gfull = (
        buf[k] for k in ("final", "whole", "term", "gp", "gin", "gx", "gfull")
    )
    pair_send, pair_recv, x_send, x_recv = (
        buf[k] for k in ("pair_send", "pair_recv", "x_send", "x_recv")
    )
    g_ref, s_ref, p_ref, t_ref, load = (buf[k] for k in ("g", "s", "p", "t", "load"))
    env = dict(coords=coords, core=core, send=buf["send"], recv=buf["recv"], sent=[], count=0)

    def at(axis, shift):
        return lax.rem(coords[axis] + shift, RING)

    grads_in = [
        pltpu.make_async_copy(grads_ref, g_ref.at[0:NBLK], load.at[0]),
        pltpu.make_async_copy(other_ref, g_ref.at[NBLK : 2 * NBLK], load.at[1]),
    ]

    def basis_in(y, z, slot):
        return pltpu.make_async_copy(basis_ref.at[:, y, z], s_ref.at[slot], load.at[2 + slot])

    def compute(turn, part):
        step = STEPS[turn]
        z = at(2, step)
        shifts = STEPS[2 * part : 2 * part + 2]

        def body(i, carry):
            y = lax.rem(coords[1] + shifts[0] + i * (shifts[1] - shifts[0]), RING)
            basis_in(y, z, i).wait()

            @pl.when(i == 0)
            def _():
                basis_in(at(1, shifts[1]), z, 1).start()

            if turn < 3 or part == 0:
                z_next = z if part == 0 else at(2, STEPS[turn + 1])

                @pl.when(i == 1)
                def _():
                    basis_in(at(1, STEPS[2 - 2 * part]), z_next, 0).start()

            e = 4 * y + z
            blocks = [slot_ref[4 * e + j] for j in range(4)]

            def rows(lo, hi):
                return jnp.concatenate([g_ref[b, :, lo:hi] for b in blocks], axis=0)

            acc = mm_nt(rows(0, QUARTER), s_ref[i, 0])
            for x in range(1, 4):
                acc += mm_nt(rows(x * QUARTER, (x + 1) * QUARTER), s_ref[i, x])
            place = lax.broadcasted_iota(jnp.int32, acc.shape, 0) // BLOCK
            p_ref[...] = jnp.where(place < count_ref[e], acc, 0.0).T.astype(jnp.bfloat16)
            for c in range(N_DP):
                value = mm(p_ref[...], rows(c * COLS, (c + 1) * COLS))
                cols = slice((c % 2) * COLS, (c % 2 + 1) * COLS)
                t_ref[step, 2 * part + i, c // 2, :, cols] = value.astype(jnp.bfloat16)
            return carry

        lax.fori_loop(0, 2, body, 0)

    def first_ring(k, slot, step, part):
        row, count = PARTS[k]
        rows = pl.ds(row, count)
        base = 2 * part

        def held(shift, half):
            cols = cols_of_half(half)
            if k == 0:
                return t_ref.at[step, base : base + 2, at(0, shift), rows, cols]
            if k == 1:
                return t_ref.at[step, PLACE[shift], :, rows, cols]
            return t_ref.at[shift, base : base + 2, :, rows, cols]

        def store(half, index, value):
            if k == 0:
                place = (step, base + index[0], coords[0])
            elif k == 1:
                place = (step, PLACE[0], index[0])
            else:
                place = (0, base + index[0], index[1])
            t_ref[(*place, rows, cols_of_half(half))] = value.astype(jnp.bfloat16)

        far, near = buf["far1", k].at[slot], buf["near1", k].at[slot]
        return ReduceRing(env, k, ((2,), (4,), (2, 4))[k], held, far, near, store)

    def second_ring(k):
        row, count = PARTS[k]
        rows = pl.ds(row, count)
        out = buf["sum2", k]

        def held(shift, half):
            cols = cols_of_half(half)
            if k == 0:
                return t_ref.at[shift, :, coords[0], rows, cols]
            if k == 1:
                return t_ref.at[shift, PLACE[0], :, rows, cols]
            return t_ref.at[0, :, at(0, shift), rows, cols]

        def store(half, index, value):
            out[(*index, ALL, cols_of_half(half))] = value

        return ReduceRing(env, AXES[k][1], (4,), held, buf["far2", k], buf["near2", k], store)

    def third_ring(k):
        row, count = PARTS[k]
        axis = AXES[k][2]

        def held(shift, half):
            place = PLACE[shift] if axis == 1 else at(axis, shift)
            return buf["sum2", k].at[place, :, cols_of_half(half)]

        def store(half, index, value):
            final[row : row + count, half * COLS : (half + 1) * COLS] = value

        return ReduceRing(env, axis, (), held, buf["far3", k], buf["near3", k], store)

    xs = [[first_ring(0, 2 * t + h, STEPS[t], h) for h in range(2)] for t in range(4)]
    ys = [first_ring(1, t, STEPS[t], 0) for t in range(4)]
    zs = [first_ring(2, h, None, h) for h in range(2)]
    second = [second_ring(k) for k in range(3)]
    third = [third_ring(k) for k in range(3)]

    for c in grads_in:
        c.start()
    basis_in(at(1, STEPS[0]), at(2, STEPS[0]), 0).start()
    whole_own = pltpu.make_async_copy(
        basis_ref.at[:, coords[1], coords[2]], whole.at[core], load.at[4]
    )
    meet(coords, core)
    for c in grads_in:
        c.wait()

    def run(rings, method):
        for ring in rings:
            method(ring)

    def batch(turn, part):
        compute(turn, part)
        xs[turn][part].begin()
        if part == 0:
            ys[turn].send_far()
            ys[turn].send_right()
        else:
            ys[turn].send_left()
        if turn < 3:
            (ReduceRing.send_far, ReduceRing.send_right, ReduceRing.send_left)[turn](zs[part])

    forward, finish = ReduceRing.forward, ReduceRing.finish
    batch(0, 0)
    batch(0, 1)
    batch(1, 0)
    xs[0][0].forward()
    batch(1, 1)
    xs[0][1].forward()
    ys[0].forward()
    zs[0].forward_half(0)
    batch(2, 0)
    zs[1].forward_half(0)
    xs[1][0].forward()
    whole_own.start()
    whole_swap = pltpu.make_async_remote_copy(
        basis_ref.at[:, coords[1], coords[2]],
        whole.at[core],
        pair_send.at[8],
        pair_recv.at[8],
        device(coords, 1 - core),
        MESH,
    )
    whole_swap.start()
    batch(2, 1)
    zs[0].forward_half(1)
    xs[1][1].forward()
    ys[1].forward()
    run(xs[0], finish)
    ys[0].finish()
    run(second[:2], ReduceRing.send_far)
    batch(3, 0)
    zs[1].forward_half(1)
    xs[2][0].forward()
    whole_own.wait()
    whole_swap.wait()
    gp[...] = jnp.zeros_like(gp)
    for x in range(4):
        for h in range(2):
            gp[h * HALF : (h + 1) * HALF, 0:HALF] += mm_nt(whole[h, x], whole[0, x])
            gp[h * HALF : (h + 1) * HALF, HALF:] += mm_nt(whole[h, x], whole[1, x])
    batch(3, 1)
    xs[2][1].forward()
    ys[2].forward()
    run(xs[1], finish)
    ys[1].finish()
    run(second[:2], ReduceRing.send_right)
    run(xs[3], forward)
    ys[3].forward()
    run(zs, finish)
    second[2].begin()
    run(xs[2], finish)
    ys[2].finish()
    run(second[:2], ReduceRing.send_left)
    run(second, forward)
    run(xs[3], finish)
    ys[3].finish()
    for k in (2, 0, 1):
        second[k].finish()
        third[k].begin()
    for k in (2, 0, 1):
        third[k].forward()
    run(third, finish)
    sent = env["sent"]
    partner = device(coords, 1 - core)
    mine = pl.ds(pl.multiple_of(core * HALF, HALF), HALF)
    theirs = pl.ds(pl.multiple_of((1 - core) * HALF, HALF), HALF)

    def give(src, dst, which):
        c = pltpu.make_async_remote_copy(
            src, dst, pair_send.at[which], pair_recv.at[which], partner, MESH
        )
        c.start()
        return c

    def across(src, dst, which, by):
        c = pltpu.make_async_remote_copy(
            src, dst, x_send.at[which], x_recv.at[which], device(moved(coords, 0, by), core), MESH
        )
        c.start()
        return c

    here = pl.ds(pl.multiple_of(core * COLS, COLS), COLS)
    there = pl.ds(pl.multiple_of((1 - core) * COLS, COLS), COLS)
    swap = give(final.at[:, there], term.at[mine], 0)
    term[mine, :] = final[:, here]
    product = two_pass(gp[...], sketch_ref[...])
    swap.wait()
    average = float(BLOCK * NBLK * N_DP)
    unscaled = product + term[...] / average
    term[...] = unscaled
    gp[...] = three_pass_nt(unscaled, unscaled)
    swap = give(gp.at[theirs], gin, 1)
    swap.wait()
    gin[...] = gin[...] + gp[mine, :]
    quarter = HALF // 2
    right = across(gin.at[0:quarter], gx.at[0, 0:quarter], 0, 1)
    left = across(gin.at[quarter:HALF], gx.at[1, quarter:HALF], 1, 3)
    right_rest = across(gin.at[quarter:HALF], gx.at[0, quarter:HALF], 10, 1)
    left_rest = across(gin.at[0:quarter], gx.at[1, 0:quarter], 11, 3)
    right.wait_recv()
    on_right = across(gx.at[0, 0:quarter], gx.at[2, 0:quarter], 2, 1)
    left.wait_recv()
    on_left = across(gx.at[1, quarter:HALF], gx.at[2, quarter:HALF], 3, 3)
    for c in (right, left):
        c.wait_send()
    for c in (right_rest, left_rest, on_right, on_left):
        c.wait()
    gfull[mine, :] = (gin[...] + gx[2]) + (gx[0] + gx[1])
    swap = give(gfull.at[mine], gfull.at[mine], 2)
    swap.wait()
    gram = gfull[...]
    row = lax.broadcasted_iota(jnp.int32, (L, L), 0)
    col = lax.broadcasted_iota(jnp.int32, (L, L), 1)
    diagonal = row == col
    total = jnp.sum(jnp.where(diagonal, gram, 0.0)) + EPSILON
    total = jnp.full((1, 1), total, jnp.float32)
    a = gram / total
    q = None
    for step in range(ITERS):
        p = jnp.where(diagonal, 1.5, 0.0) - 0.5 * a
        q = p if q is None else three_pass(p, q)
        if step < ITERS - 1:
            a = three_pass(three_pass(p, a), p)
    scale = D**0.5 * lax.rsqrt(total)
    factor = three_pass(q, term[...] * scale)

    def chunk(shift, core_of):
        index = 2 * lax.rem(coords[0] + shift, RING) + core_of
        return pl.ds(pl.multiple_of(index * COLS, COLS), COLS)

    def piece(shift, rows=slice(None)):
        return out_ref.at[rows, chunk(shift, core)]

    out_ref[:, chunk(0, core)] = factor.astype(jnp.bfloat16)
    upper, lower = pl.ds(0, HALF), pl.ds(HALF, HALF)
    right = across(piece(0, upper), piece(0, upper), 4, 1)
    left = across(piece(0, lower), piece(0, lower), 6, 3)
    right_rest = across(piece(0, lower), piece(0, lower), 5, 1)
    left_rest = across(piece(0, upper), piece(0, upper), 7, 3)
    gives = [give(piece(0), piece(0), 3)]
    right.wait_recv()
    on_right = across(piece(3, upper), piece(3, upper), 8, 1)
    left.wait_recv()
    on_left = across(piece(1, lower), piece(1, lower), 9, 3)
    right_rest.wait_recv()
    gives.append(give(piece(3), piece(3), 4))
    left_rest.wait_recv()
    gives.append(give(piece(1), piece(1), 5))
    on_right.wait_recv()
    gives.append(give(piece(2, upper), piece(2, upper), 6))
    on_left.wait_recv()
    gives.append(give(piece(2, lower), piece(2, lower), 7))
    for c in (right, left, right_rest, left_rest, on_right, on_left):
        c.wait_send()
    for c in gives:
        c.wait()
    for c in sent:
        c.wait_send()


def split(a):
    high = a.astype(jnp.bfloat16)
    return high, (a - high.astype(jnp.float32)).astype(jnp.bfloat16)


def mm(a, b):
    return jnp.dot(a, b, preferred_element_type=jnp.float32)


def two_pass(a, b):
    high, low = split(a)
    return mm(high, b) + mm(low, b)


def three_pass(a, b):
    ah, al = split(a)
    bh, bl = split(b)
    return mm(ah, bh) + (mm(ah, bl) + mm(al, bh))


def three_pass_nt(a, b):
    ah, al = split(a)
    bh, bl = split(b)
    return mm_nt(ah, bh) + (mm_nt(ah, bl) + mm_nt(al, bh))


def reduce_terms(count, slots, grads, other, basis, own):
    buffers = reduce_buffers()
    smem, vmem, where = (
        pl.BlockSpec(memory_space=m) for m in (pltpu.SMEM, pltpu.VMEM, pl.ANY)
    )
    return pl.pallas_call(
        functools.partial(reduce_kernel, tuple(buffers)),
        out_shape=jax.ShapeDtypeStruct((L, D), jnp.bfloat16),
        in_specs=[smem, smem, where, where, where, vmem],
        out_specs=vmem,
        scratch_shapes=list(buffers.values()),
        compiler_params=pltpu.CompilerParams(
            collective_id=1, has_side_effects=True, vmem_limit_bytes=67043328
        ),
    )(count, slots, grads, other, basis, own)


def shards(grads, block_expert, sketch):
    own = sketch[0]
    owners = block_expert[:, 0]
    theirs = lax.ppermute(owners, "dp", [(k, k ^ 1) for k in range(N_DP)])
    grads = grads.reshape(NBLK, BLOCK, D)
    basis, other = gather(own, grads)
    count, slots = slot_table(jnp.concatenate([owners, theirs]))
    return reduce_terms(count, slots, grads, other, basis, own)[None]


def solution(mesh):
    in_specs = (P(("dp", "expert"), None), P(("dp", "expert"), None), P("expert", None, "dp"))
    out_specs = P("expert", None, None)
    return jax.shard_map(shards, mesh=mesh, in_specs=in_specs, out_specs=out_specs, check_vma=False)
```
